128 devices in a mesh: gx: 4 (over x_hi, core), gy: 4 (over y), gz: 8 (over z, x_lo).
Axes of the slice: x: 4 (x_hi: 2, x_lo: 2; x = x_hi * 2 + x_lo), y: 4, z: 4, core: 2. Of those that a mesh axis runs over, the one named last changes fastest.
Arguments:
- field: float32 [64, 1024, 1024], P('gx', 'gy', 'gz'), may hold values from -6 to 6
- source: float32 [64, 1024, 1024], P('gx', 'gy', 'gz'), may hold values from -6 to 6
Outputs:
- smoothed: float32 [64, 1024, 1024], P('gx', 'gy', 'gz')
The draws below stay inside these ranges and needn't reach their ends.
All inputs are finite; a program needn't handle non-finite values.
Results may differ from the reference program's by a relative error of at most 0.00002.
Values sent between devices are 32-bit elements; how exact they have to be, the bound alone decides.
No kernel may reach another device: no remote copies, remote signals or barrier semaphores. Data moves between devices by JAX's collectives and lax.ppermute only.
A program may use at most 64 MiB of HBM per device.

```python
import jax
import jax.numpy as jnp

SWEEPS = 3
NX = 64
NY = 1024
NZ = 1024


def block_levels(key, shape, split, least, top_value):
    def one(position, parts):
        draws = jax.random.uniform(jax.random.fold_in(jax.random.fold_in(key, 6), position), (parts,), jnp.float32, least / len(split), top_value / len(split))
        return jnp.repeat(jnp.exp(draws), shape[position] // parts).reshape((-1,) + (1,) * (len(shape) - position - 1))

    loudness = one(*split[0])
    for cut in split[1:]:
        loudness = loudness * one(*cut)
    return loudness


def bell_draw(own_key, shape, spread, most, shards=(), held_as=jnp.bfloat16):
    entries = jax.random.normal(own_key, shape, jnp.float32) * spread
    if len(shards) > 0:
        entries = block_levels(own_key, shape, shards, -0.22, 0.18) * entries
    return jnp.clip(entries, min=-most, max=most).astype(held_as)


def setup_inputs(seed: int = 0) -> dict:
    key_of = jax.random.split(jax.random.key(seed), 3)
    field = bell_draw(key_of[0], (NX, NY, NZ), 1.0, 6.0, ((0, 4), (1, 4), (2, 8)), jnp.float32)
    source = bell_draw(key_of[1], (NX, NY, NZ), 1.0, 6.0, ((0, 4), (1, 4), (2, 8)), jnp.float32)
    return dict(field=field, source=source)


def relax(values, source, parity, colour):
    padded = jnp.pad(values, ((1, 1), (0, 0), (0, 0)))
    beside = padded[2:] + padded[:-2]
    beside = beside + jnp.roll(values, -1, 1) + jnp.roll(values, 1, 1)
    beside = beside + jnp.roll(values, -1, 2) + jnp.roll(values, 1, 2)
    return jnp.where(parity == colour, (source + beside) / 6.0, values)


def reference(field, source):
    nx, ny, nz = field.shape
    parity = (jnp.arange(nx, dtype=jnp.int32)[:, None, None] + jnp.arange(ny, dtype=jnp.int32)[None, :, None] + jnp.arange(nz, dtype=jnp.int32)[None, None, :]) % 2
    values = field
    for sweep in range(SWEEPS):
        values = relax(values, source, parity, 0)
        values = relax(values, source, parity, 1)
    return values
```

```python
import jax
import jax.numpy as jnp
from jax import lax
from jax.experimental import pallas as pl
from jax.experimental.pallas import tpu as pltpu
from jax.sharding import PartitionSpec as P

F32 = jnp.float32
VM = pltpu.VMEM
Q, NY, NZ = 8, 256, 128
ROWS = NY + 32
TILES = NY // 8
SIXTH = 1.0 / 6.0
SUB = 8


def lanes_of():
    return lax.broadcasted_iota(jnp.int32, (8, 128), 1)


def odd_cells():
    return (lax.broadcasted_iota(jnp.int32, (8, 128), 0) + lanes_of()) % 2


def turn(value, shift):
    shift = shift % 128
    return value if shift == 0 else pltpu.roll(value, shift, 1)


def mirrored(q, flip):
    return q + flip * (Q - 1 - 2 * q)


CHUNKS = 4


def pack_kernel(flip_ref, field, source, bm, srm, sbm, high, low, zlow, zhigh, fbuf, sbuf, sems):
    flip = flip_ref[0]
    span = NY // CHUNKS
    copies = []
    for c in range(CHUNKS):
        rows = pl.ds(c * span, span)
        for n, (src, dst) in enumerate(((field, fbuf), (source, sbuf))):
            copy = pltpu.make_async_copy(src.at[:, :, rows, :], dst.at[:, :, rows, :], sems.at[2 * c + n])
            copy.start()
            copies.append(copy)
    odd = odd_cells() == 1
    lane = lanes_of()
    col = lane % 16
    left_half = lane < 64

    def tile(t, carry):
        r = pl.multiple_of(t * 8, 8)
        rows = pl.ds(r, 8)
        put = pl.ds(pl.multiple_of(r + 16, 8), 8)
        acc = [jnp.zeros((8, 128), F32)] * 4
        for q in range(Q):
            at = mirrored(q, flip)
            f0, f1 = fbuf[at, 0, rows, :], fbuf[at, 1, rows, :]
            s0, s1 = sbuf[at, 0, rows, :], sbuf[at, 1, rows, :]
            b = jnp.where(odd, f0, f1)
            sr = jnp.where(odd, s1, s0)
            sb = jnp.where(odd, s0, s1)
            bm[q, put, :] = b
            srm[q, put, :] = sr
            sbm[q, put, :] = sb
            for out, d in ((low, q), (high, Q - 1 - q)):
                if d < 3:
                    out[d, rows, :] = b
                    out[3 + d, rows, :] = sr
                if d < 2:
                    out[6 + d, rows, :] = sb
            here = lane // 16 == q
            parts = (
                turn(b, 16 * q),
                turn(jnp.where(left_half, sr, b), 16 * q + 6),
                turn(jnp.where(left_half, sb, sr), 16 * q + 11),
                turn(sb, 16 * q + 15),
            )
            acc = [jnp.where(here, new, old) for new, old in zip(parts, acc)]
        zlow[rows, :] = jnp.where(col < 6, acc[0], jnp.where(col < 11, acc[1], acc[2]))
        zhigh[rows, :] = jnp.where(col < 6, acc[1], jnp.where(col < 11, acc[2], acc[3]))
        return carry

    for c in range(CHUNKS):
        copies[2 * c].wait()
        copies[2 * c + 1].wait()
        lax.fori_loop(c * span // 8, (c + 1) * span // 8, tile, 0)


def y_kernel(bm, srm, sbm, zr, zl, ylow, yhigh):
    for out, row in ((ylow, 0), (yhigh, NY - 8)):
        for n, ref in enumerate((bm, srm, sbm)):
            for q in range(Q):
                out[8 * n + q] = ref[q, row + 16:row + 24, :]
        out[24] = zr[row:row + 8, :]
        out[25] = zl[row:row + 8, :]


def corner_kernel(yr, yl, zr, zl, high, low):
    lane = lanes_of()
    left_half = lane < 64
    for out, planes in ((low, (0, 1, 2)), (high, (7, 6, 5))):
        for side, ref in enumerate((yr, yl)):
            for d, q in enumerate(planes):
                out[8 * side + d] = ref[q]
                out[8 * side + 3 + d] = ref[8 + q]
                if d < 2:
                    out[8 * side + 6 + d] = ref[16 + q]

    def put(n, r, l):
        low[n] = jnp.where(left_half, r, turn(l, 64))
        high[n] = jnp.where(left_half, turn(r, 48), turn(l, 112))

    def tile(t, carry):
        rows = pl.ds(pl.multiple_of(t * 8, 8), 8)
        put(t + 17, zr[rows, :], zl[rows, :])
        return carry

    put(16, yl[24], yl[25])
    put(49, yr[24], yr[25])
    lax.fori_loop(0, TILES, tile, 0)


def mirror_jobs(jobs):
    swap = {"both": "both", "up": "down", "down": "up"}
    return [(Q - 1 - q, swap[x], None if keep is None else 1 - keep) for q, x, keep in jobs]


def half_sweep(r, red, jobs, odd, lane, get, factor, rims=True):
    first, last = lane == 0, lane == 127
    rows = pl.ds(r, 8)
    above, below = pl.ds(r - 1, 8), pl.ds(r + 1, 8)
    centre = {}

    def at(q):
        if q not in centre:
            main, rim = get("black" if red else "red", q)
            centre[q] = (main[rows, :], rim[rows, :] if rims else None)
        return centre[q]

    done = {}
    for q, x, keep in jobs:
        mains = get("black" if red else "red", q)
        sources = get("sr" if red else "sb", q)
        olds = get("red" if red else "black", q)
        cm = at(q)[0]
        ch = at(q)[1] if rims else mains[1][rows, :]
        lm, lh = turn(cm, 1), turn(ch, 1)
        rm, rh = turn(cm, 127), turn(ch, 127)
        beside = (
            jnp.where(first, lh, lm) + jnp.where(last, rh, rm),
            jnp.where(first, lm, lh) + jnp.where(last, rm, rh) if rims else None,
        )
        new = []
        for n in range(2 if rims else 1):
            if x == "up":
                along = at(q + 1)[n]
            elif x == "down":
                along = at(q - 1)[n]
            elif red:
                along = jnp.where(odd, at(q + 1)[n], at(q - 1)[n])
            else:
                along = jnp.where(odd, at(q - 1)[n], at(q + 1)[n])
            total = (sources[n][rows, :] + at(q)[n]) + (along + beside[n])
            total = total + (mains[n][above, :] + mains[n][below, :])
            value = total * factor(q)
            if keep == 1:
                value = jnp.where(odd, olds[n][rows, :], value)
            elif keep == 0:
                value = jnp.where(odd, value, olds[n][rows, :])
            new.append(value)
        done[q] = new
    return done


def sweep_rows(red, jobs, odd, lane, get, factor):
    def tile(t, carry):
        r = pl.multiple_of(t * 8 + 8, 8)
        for q, new in half_sweep(r, red, jobs, odd, lane, get, factor).items():
            for ref, value in zip(get("red" if red else "black", q), new):
                ref[pl.ds(r, 8), :] = value
        return carry

    lax.fori_loop(0, TILES + 2, tile, 0)


def full(*qs):
    return [(q, "both", None) for q in qs]


def inner_kernel(flip_ref, bm_in, srm_in, sbm_in, yr, yl, zr, zl, bm, rm, srm, sbm, bh, rh, srh, sbh):
    del bm_in, srm_in, sbm_in
    lane = lanes_of()
    odd = (odd_cells() + flip_ref[0]) % 2 == 1
    col = lane % 16

    for row, ref in ((8, yl), (NY + 16, yr)):
        for q in range(Q):
            bm[q, row:row + 8, :] = ref[q]
            srm[q, row:row + 8, :] = ref[8 + q]
            sbm[q, row:row + 8, :] = ref[16 + q]

    def rim(rows, r, l):
        one = jnp.where(col < 6, l, r)
        two = jnp.where(col < 11, l, r)
        for q in range(Q):
            parts = [turn(r, -16 * q), turn(one, -16 * q - 6), turn(two, -16 * q - 11), turn(l, 113 - 16 * q)]
            for n, (ref, width) in enumerate(((bh, 6), (srh, 5), (sbh, 4))):
                ref[q, rows, :] = jnp.where(lane < width, parts[n], jnp.where(lane >= 128 - width, parts[n + 1], 0.0))

    rim(pl.ds(8, 8), yl[24], yl[25])
    rim(pl.ds(NY + 16, 8), yr[24], yr[25])

    def tile(t, carry):
        r = pl.multiple_of(t * 8, 8)
        rim(pl.ds(pl.multiple_of(r + 16, 8), 8), zr[pl.ds(r, 8), :], zl[pl.ds(r, 8), :])
        return carry

    lax.fori_loop(0, TILES, tile, 0)

    table = {"black": (bm, bh), "red": (rm, rh), "sr": (srm, srh), "sb": (sbm, sbh)}

    def get(kind, q):
        return [ref.at[q] for ref in table[kind]]

    def factor(q):
        return SIXTH

    edge1, edge3, edge5 = [(0, "up", None)], [(1, "up", 0)], [(2, "up", 0)]
    for red, jobs in (
        (True, edge1 + full(*range(1, 7)) + mirror_jobs(edge1)),
        (False, full(*range(1, 7))),
        (True, edge3 + full(*range(2, 6)) + mirror_jobs(edge3)),
        (False, full(*range(2, 6))),
        (True, edge5 + full(3, 4) + mirror_jobs(edge5)),
        (False, full(3, 4)),
    ):
        sweep_rows(red, jobs, odd, lane, get, factor)


OUT_CHUNKS = 4


def outer_kernel(flip_ref, wall_ref, bm_in, rm_in, srm, sbm, bh_in, rh_in, srh, sbh, high, low, chigh, clow,
                 out, bm, rm, bh, rh, xbm, xbh, xrm, xrh, xsrm, xsrh, xsbm, xsbh, obuf, sems):
    del bm_in, rm_in, bh_in, rh_in
    flip = flip_ref[0]
    wall = wall_ref[0]
    lane = lanes_of()
    plain = odd_cells() == 1
    odd = (odd_cells() + flip) % 2 == 1

    for side, main, corner in ((0, low, clow), (1, high, chigh)):
        for d in range(3):
            slot = 3 * side + d
            for n, (ref, deep) in enumerate(((xbm, 3), (xsrm, 3), (xsbm, 2))):
                if d < deep:
                    slot_n = deep * side + d
                    ref[slot_n, 8:16, :] = corner[8 + 3 * n + d]
                    ref[slot_n, 16:NY + 16, :] = main[3 * n + d]
                    ref[slot_n, NY + 16:NY + 24, :] = corner[3 * n + d]

    def rim(t, carry):
        rows = pl.ds(pl.multiple_of(t * 8 + 8, 8), 8)
        for side, corner in ((0, clow), (1, chigh)):
            both = corner[16 + t]
            for d in range(3):
                c = 16 * (d if side == 0 else 2 - d)
                for n, (ref, deep, width) in enumerate(((xbh, 3, 6), (xsrh, 3, 5), (xsbh, 2, 4))):
                    if d < deep:
                        off = c + (0, 6, 11)[n]
                        right = turn(both, -off)
                        left = turn(both, 128 - width - 64 - off)
                        ref[deep * side + d, rows, :] = jnp.where(
                            lane < width, right, jnp.where(lane >= 128 - width, left, 0.0)
                        )
        return carry

    lax.fori_loop(0, TILES + 2, rim, 0)

    own = {"black": (bm, bh), "red": (rm, rh), "sr": (srm, srh), "sb": (sbm, sbh)}
    halo = {"black": (xbm, xbh), "red": (xrm, xrh), "sr": (xsrm, xsrh), "sb": (xsbm, xsbh)}

    def get(kind, q):
        if 0 <= q < Q:
            return [ref.at[q] for ref in own[kind]]
        deep = 2 if kind == "sb" else 3
        slot = -1 - q if q < 0 else deep + q - Q
        return [ref.at[slot] for ref in halo[kind]]

    def factor(q):
        return wall if q < 0 else SIXTH

    for red, jobs in (
        (True, [(-3, "up", None)] + full(-2, -1) + [(0, "down", 1)]),
        (False, full(-2, -1, 0)),
        (True, [(-2, "up", None)] + full(-1, 0) + [(1, "down", 1)]),
        (False, full(-1, 0, 1)),
        (True, [(-1, "up", None)] + full(0, 1) + [(2, "down", 1)]),
    ):
        sweep_rows(red, jobs + mirror_jobs(jobs), odd, lane, get, factor)

    jobs = full(0, 1, 2)
    jobs = jobs + mirror_jobs(jobs)

    def tile(t, carry):
        r = pl.multiple_of(t * 8 + 16, 8)
        rows = pl.ds(pl.multiple_of(t * 8, 8), 8)
        new = half_sweep(r, False, jobs, odd, lane, get, factor, rims=False)
        for q in range(Q):
            b = new[q][0] if q in new else bm[q, pl.ds(r, 8), :]
            v = rm[q, pl.ds(r, 8), :]
            at = mirrored(q, flip)
            obuf[at, 0, rows, :] = jnp.where(plain, b, v)
            obuf[at, 1, rows, :] = jnp.where(plain, v, b)
        return carry

    span = NY // OUT_CHUNKS
    copies = []
    for c in range(OUT_CHUNKS):
        lax.fori_loop(c * span // 8, (c + 1) * span // 8, tile, 0)
        rows = pl.ds(c * span, span)
        copy = pltpu.make_async_copy(obuf.at[:, :, rows, :], out.at[:, :, rows, :], sems.at[c])
        copy.start()
        copies.append(copy)
    for copy in copies:
        copy.wait()


def smem():
    return pl.BlockSpec(memory_space=pltpu.SMEM)


def vmem(n):
    return [pl.BlockSpec(memory_space=VM)] * n


def hbm():
    return pl.BlockSpec(memory_space=pl.ANY)


def near(*values):
    return [pltpu.with_memory_space_constraint(v, VM) for v in values]


def room(mib):
    return pltpu.CompilerParams(vmem_limit_bytes=mib * 1024 * 1024)


def ring(size, step):
    return [(i, (i + step) % size) for i in range(size)]


def on_device(field, source):
    gx = lax.axis_index("gx")
    flip = (gx % 2).astype(jnp.int32)[None]
    last = lax.axis_size("gx") - 1
    wall = jnp.where((gx == 0) | (gx == last), 0.0, SIXTH).astype(F32)[None]
    pairs = lax.axis_size("gx") // 2
    chip = [p for i in range(pairs) for p in ((2 * i, 2 * i + 1), (2 * i + 1, 2 * i))]
    across = [p for i in range(pairs - 1) for p in ((2 * i + 1, 2 * i + 2), (2 * i + 2, 2 * i + 1))]
    ny, nz = lax.axis_size("gy"), lax.axis_size("gz")

    fields, sources = [
        pltpu.with_memory_space_constraint(a.reshape(Q, 2, NY, NZ), pltpu.HBM) for a in (field, source)
    ]
    work = VM((Q, ROWS, NZ), F32)
    face = VM((Q, NY, NZ), F32)
    bm, srm, sbm, high, low, zlow, zhigh = pl.pallas_call(
        pack_kernel,
        name="pack", compiler_params=room(8),
        out_shape=(work, work, work, face, face, VM((NY, NZ), F32), VM((NY, NZ), F32)),
        in_specs=[smem(), hbm(), hbm()],
        out_specs=vmem(7),
        scratch_shapes=[VM((Q, 2, NY, NZ), F32), VM((Q, 2, NY, NZ), F32), pltpu.SemaphoreType.DMA((2 * CHUNKS,))],
    )(flip, fields, sources)

    high = lax.ppermute(high, "gx", chip)
    low = lax.ppermute(low, "gx", across)
    zr = lax.ppermute(zlow, "gz", ring(nz, -1))
    zl = lax.ppermute(zhigh, "gz", ring(nz, 1))
    bm, srm, sbm, zr, zl = near(bm, srm, sbm, zr, zl)
    strip = VM((26, 8, NZ), F32)
    ylow, yhigh = pl.pallas_call(
        y_kernel, name="yfaces", compiler_params=room(2), out_shape=(strip, strip), in_specs=vmem(5), out_specs=vmem(2)
    )(bm, srm, sbm, zr, zl)
    yr = lax.ppermute(ylow, "gy", ring(ny, -1))
    yl = lax.ppermute(yhigh, "gy", ring(ny, 1))
    yr, yl = near(yr, yl)
    corner = VM((50, 8, NZ), F32)
    chigh, clow = pl.pallas_call(
        corner_kernel, name="corners", compiler_params=room(2), out_shape=(corner, corner), in_specs=vmem(4), out_specs=vmem(2)
    )(yr, yl, zr, zl)
    chigh = lax.ppermute(chigh, "gx", chip)
    clow = lax.ppermute(clow, "gx", across)

    zr, zl, yr, yl = near(zr, zl, yr, yl)
    bm, rm, srm, sbm, bh, rh, srh, sbh = pl.pallas_call(
        inner_kernel,
        name="inner", compiler_params=room(4),
        out_shape=(work,) * 8,
        in_specs=[smem()] + vmem(7),
        out_specs=vmem(8),
        input_output_aliases={1: 0, 2: 2, 3: 3},
    )(flip, bm, srm, sbm, yr, yl, zr, zl)

    args = near(bm, rm, srm, sbm, bh, rh, srh, sbh, high, low, chigh, clow)
    halo3, halo2 = VM((6, ROWS, NZ), F32), VM((4, ROWS, NZ), F32)
    out = pl.pallas_call(
        outer_kernel,
        name="outer", compiler_params=room(16),
        out_shape=(jax.ShapeDtypeStruct((Q, 2, NY, NZ), F32),) + (work,) * 4,
        in_specs=[smem(), smem()] + vmem(12),
        out_specs=[hbm()] + vmem(4),
        input_output_aliases={2: 1, 3: 2, 6: 3, 7: 4},
        scratch_shapes=[halo3] * 6 + [halo2] * 2 + [VM((Q, 2, NY, NZ), F32), pltpu.SemaphoreType.DMA((OUT_CHUNKS,))],
    )(flip, wall, *args)[0]
    return out.reshape(field.shape)


def solution(mesh):
    spec = P("gx", "gy", "gz")
    return jax.shard_map(on_device, mesh=mesh, in_specs=(spec, spec), out_specs=spec, check_vma=False)
```

```python
import jax
import jax.numpy as jnp
from jax import lax
from jax.experimental import pallas as pl
from jax.experimental.pallas import tpu as pltpu
from jax.sharding import PartitionSpec as P


F32 = jnp.float32
VM = pltpu.VMEM
Q, NY, NZ = 8, 256, 128
ROWS = NY + 32
TILES = NY // 8
SIXTH = 1.0 / 6.0


def lanes_of():
    return lax.broadcasted_iota(jnp.int32, (8, 128), 1)


def odd_cells():
    return (lax.broadcasted_iota(jnp.int32, (8, 128), 0) + lanes_of()) % 2


def turn(value, shift):
    shift = shift % 128
    return value if shift == 0 else pltpu.roll(value, shift, 1)


def mirrored(q, flip):
    return q + flip * (Q - 1 - 2 * q)


BATCH = 40


def batched(count, size, body):
    def step(i, carry):
        body(i * size, size)
        return carry

    lax.fori_loop(0, count // size, step, 0)
    if count % size:
        body(count - count % size, count % size)


CHUNKS = 4


def pack_kernel(flip_ref, field, source, bm, srm, sbm, zlow, zhigh, fbuf, sbuf, sems):
    flip = flip_ref[0] % 2
    span = NY // CHUNKS
    copies = []
    for c in range(CHUNKS):
        rows = pl.ds(c * span, span)
        for n, (src, dst) in enumerate(((field, fbuf), (source, sbuf))):
            copy = pltpu.make_async_copy(src.at[:, :, rows, :], dst.at[:, :, rows, :], sems.at[2 * c + n])
            copy.start()
            copies.append(copy)
    odd = odd_cells() == 1
    lane = lanes_of()
    col = lane % 16
    left_half = lane < 64

    def tile(t):
        r = pl.multiple_of(t * 8, 8)
        rows = pl.ds(r, 8)
        put = pl.ds(pl.multiple_of(r + 16, 8), 8)
        acc = [jnp.zeros((8, 128), F32)] * 4
        for q in range(Q):
            at = mirrored(q, flip)
            f0, f1 = fbuf[at, 0, rows, :], fbuf[at, 1, rows, :]
            s0, s1 = sbuf[at, 0, rows, :], sbuf[at, 1, rows, :]
            b = jnp.where(odd, f0, f1)
            sr = jnp.where(odd, s1, s0)
            sb = jnp.where(odd, s0, s1)
            bm[q, put, :] = b
            srm[q, put, :] = sr
            sbm[q, put, :] = sb
            here = lane // 16 == q
            parts = (
                turn(b, 16 * q),
                turn(jnp.where(left_half, sr, b), 16 * q + 6),
                turn(jnp.where(left_half, sb, sr), 16 * q + 11),
                turn(sb, 16 * q + 15),
            )
            acc = [jnp.where(here, new, old) for new, old in zip(parts, acc)]
        zlow[rows, :] = jnp.where(col < 6, acc[0], jnp.where(col < 11, acc[1], acc[2]))
        zhigh[rows, :] = jnp.where(col < 6, acc[1], jnp.where(col < 11, acc[2], acc[3]))

    def body(i, carry):
        for u in range(4):
            tile(i * 4 + u)
        return carry

    for c in range(CHUNKS):
        copies[2 * c].wait()
        copies[2 * c + 1].wait()
        lax.fori_loop(c * span // 32, (c + 1) * span // 32, body, 0)


def face_kernel(bm, srm, sbm, high, low):
    def body(i, carry):
        rows = pl.ds(pl.multiple_of(i * 32, 32), 32)
        put = pl.ds(pl.multiple_of(i * 32 + 16, 16), 32)
        for out, planes in ((low, (0, 1, 2)), (high, (7, 6, 5))):
            for d, q in enumerate(planes):
                out[d, rows, :] = bm[q, put, :]
                out[3 + d, rows, :] = srm[q, put, :]
                if d < 2:
                    out[6 + d, rows, :] = sbm[q, put, :]
        return carry

    lax.fori_loop(0, NY // 32, body, 0)


def y_kernel(bm, srm, sbm, zr, zl, ylow, yhigh):
    for out, row in ((ylow, 0), (yhigh, NY - 8)):
        for n, ref in enumerate((bm, srm, sbm)):
            for q in range(Q):
                out[8 * n + q] = ref[q, row + 16:row + 24, :]
        out[24] = zr[row:row + 8, :]
        out[25] = zl[row:row + 8, :]


def put_rim(rows, r, l, bh, srh, sbh):
    lane = lanes_of()
    col = lane % 16
    one = jnp.where(col < 6, l, r)
    two = jnp.where(col < 11, l, r)
    for q in range(Q):
        parts = [turn(r, -16 * q), turn(one, -16 * q - 6), turn(two, -16 * q - 11), turn(l, 113 - 16 * q)]
        for n, (ref, width) in enumerate(((bh, 6), (srh, 5), (sbh, 4))):
            ref[q, rows, :] = jnp.where(lane < width, parts[n], jnp.where(lane >= 128 - width, parts[n + 1], 0.0))


def rim_kernel(zr, zl, bh, srh, sbh):
    def body(first, tiles):
        for u in range(tiles):
            r = pl.multiple_of((first + u) * 8, 8)
            put_rim(pl.ds(pl.multiple_of(r + 16, 8), 8), zr[pl.ds(r, 8), :], zl[pl.ds(r, 8), :], bh, srh, sbh)

    batched(TILES, 4, body)


def corner_kernel(yr, yl, zr, zl, bm_in, srm_in, sbm_in, bh_in, srh_in, sbh_in, high, low, bm, srm, sbm, bh, srh, sbh):
    del bm_in, srm_in, sbm_in, bh_in, srh_in, sbh_in
    lane = lanes_of()
    left_half = lane < 64
    for out, planes in ((low, (0, 1, 2)), (high, (7, 6, 5))):
        for side, ref in enumerate((yr, yl)):
            for d, q in enumerate(planes):
                out[8 * side + d] = ref[q]
                out[8 * side + 3 + d] = ref[8 + q]
                if d < 2:
                    out[8 * side + 6 + d] = ref[16 + q]

    def put(n, r, l):
        low[n] = jnp.where(left_half, r, turn(l, 64))
        high[n] = jnp.where(left_half, turn(r, 48), turn(l, 112))

    def body(first, tiles):
        for u in range(tiles):
            rows = pl.ds(pl.multiple_of((first + u) * 8, 8), 8)
            put(first + u + 17, zr[rows, :], zl[rows, :])

    put(16, yl[24], yl[25])
    put(49, yr[24], yr[25])
    batched(TILES, 16, body)
    for row, ref in ((8, yl), (NY + 16, yr)):
        for q in range(Q):
            bm[q, row:row + 8, :] = ref[q]
            srm[q, row:row + 8, :] = ref[8 + q]
            sbm[q, row:row + 8, :] = ref[16 + q]
        put_rim(pl.ds(row, 8), ref[24], ref[25], bh, srh, sbh)


def mirror_jobs(jobs):
    swap = {"both": "both", "up": "down", "down": "up"}
    return [(Q - 1 - q, swap[x], None if keep is None else 1 - keep) for q, x, keep in jobs]


def half_sweep(r, red, jobs, odd, lane, get, factor, rims=True):
    first, last = lane == 0, lane == 127
    rows = pl.ds(r, 8)
    above, below = pl.ds(r - 1, 8), pl.ds(r + 1, 8)
    centre = {}

    def at(q):
        if q not in centre:
            main, rim = get("black" if red else "red", q)
            centre[q] = (main[rows, :], rim[rows, :] if rims else None)
        return centre[q]

    done = {}
    for q, x, keep in jobs:
        mains = get("black" if red else "red", q)
        sources = get("sr" if red else "sb", q)
        olds = get("red" if red else "black", q)
        cm = at(q)[0]
        ch = at(q)[1] if rims else mains[1][rows, :]
        lm, lh = turn(cm, 1), turn(ch, 1)
        rm, rh = turn(cm, 127), turn(ch, 127)
        beside = (
            jnp.where(first, lh, lm) + jnp.where(last, rh, rm),
            jnp.where(first, lm, lh) + jnp.where(last, rm, rh) if rims else None,
        )
        new = []
        for n in range(2 if rims else 1):
            if x == "up":
                along = at(q + 1)[n]
            elif x == "down":
                along = at(q - 1)[n]
            elif red:
                along = jnp.where(odd, at(q + 1)[n], at(q - 1)[n])
            else:
                along = jnp.where(odd, at(q - 1)[n], at(q + 1)[n])
            total = (sources[n][rows, :] + at(q)[n]) + (along + beside[n])
            total = total + (mains[n][above, :] + mains[n][below, :])
            value = total * factor(q)
            if keep == 1:
                value = jnp.where(odd, olds[n][rows, :], value)
            elif keep == 0:
                value = jnp.where(odd, value, olds[n][rows, :])
            new.append(value)
        done[q] = new
    return done


def sweep_rows(red, jobs, odd, lane, get, factor):
    def body(first, tiles):
        fresh = []
        for u in range(tiles):
            r = pl.multiple_of((first + u) * 8 + 8, 8)
            fresh.append((r, half_sweep(r, red, jobs, odd, lane, get, factor)))
        for r, done in fresh:
            for q, new in done.items():
                for ref, value in zip(get("red" if red else "black", q), new):
                    ref[pl.ds(r, 8), :] = value

    batched(TILES + 2, max(1, BATCH // len(jobs)), body)


def full(*qs):
    return [(q, "both", None) for q in qs]


def inner_kernel(flip_ref, bm_in, srm, sbm, bh_in, srh, sbh, bm, rm, bh, rh):
    del bm_in, bh_in
    lane = lanes_of()
    odd = (odd_cells() + flip_ref[0] % 2) % 2 == 1

    table = {"black": (bm, bh), "red": (rm, rh), "sr": (srm, srh), "sb": (sbm, sbh)}

    def get(kind, q):
        return [ref.at[q] for ref in table[kind]]

    def factor(q):
        return SIXTH

    edge1, edge3, edge5 = [(0, "up", None)], [(1, "up", 0)], [(2, "up", 0)]
    for red, jobs in (
        (True, edge1 + full(*range(1, 7)) + mirror_jobs(edge1)),
        (False, full(*range(1, 7))),
        (True, edge3 + full(*range(2, 6)) + mirror_jobs(edge3)),
        (False, full(*range(2, 6))),
        (True, edge5 + full(3, 4) + mirror_jobs(edge5)),
        (False, full(3, 4)),
    ):
        sweep_rows(red, jobs, odd, lane, get, factor)


OUT_CHUNKS = 4


def outer_kernel(flip_ref, bm_in, rm_in, srm, sbm, bh_in, rh_in, srh, sbh, high, low, chigh, clow,
                 out, bm, rm, bh, rh, xbm, xbh, xrm, xrh, xsrm, xsrh, xsbm, xsbh, obuf, sems):
    del bm_in, rm_in, bh_in, rh_in
    flip = flip_ref[0] % 2
    wall = jnp.where(flip_ref[0] >= 2, 0.0, SIXTH)
    lane = lanes_of()
    plain = odd_cells() == 1
    odd = (odd_cells() + flip) % 2 == 1

    for side, main, corner in ((0, low, clow), (1, high, chigh)):
        for d in range(3):
            for n, (ref, deep) in enumerate(((xbm, 3), (xsrm, 3), (xsbm, 2))):
                if d < deep:
                    slot_n = deep * side + d
                    ref[slot_n, 8:16, :] = corner[8 + 3 * n + d]
                    ref[slot_n, 16:NY + 16, :] = main[3 * n + d]
                    ref[slot_n, NY + 16:NY + 24, :] = corner[3 * n + d]

    def rim(first, tiles):
        for u in range(tiles):
            t = first + u
            rows = pl.ds(pl.multiple_of(t * 8 + 8, 8), 8)
            for side, corner in ((0, clow), (1, chigh)):
                both = corner[16 + t]
                for d in range(3):
                    c = 16 * (d if side == 0 else 2 - d)
                    for n, (ref, deep, width) in enumerate(((xbh, 3, 6), (xsrh, 3, 5), (xsbh, 2, 4))):
                        if d < deep:
                            off = c + (0, 6, 11)[n]
                            right = turn(both, -off)
                            left = turn(both, 128 - width - 64 - off)
                            ref[deep * side + d, rows, :] = jnp.where(
                                lane < width, right, jnp.where(lane >= 128 - width, left, 0.0)
                            )

    batched(TILES + 2, 3, rim)

    own = {"black": (bm, bh), "red": (rm, rh), "sr": (srm, srh), "sb": (sbm, sbh)}
    halo = {"black": (xbm, xbh), "red": (xrm, xrh), "sr": (xsrm, xsrh), "sb": (xsbm, xsbh)}

    def get(kind, q):
        if 0 <= q < Q:
            return [ref.at[q] for ref in own[kind]]
        deep = 2 if kind == "sb" else 3
        slot = -1 - q if q < 0 else deep + q - Q
        return [ref.at[slot] for ref in halo[kind]]

    def factor(q):
        return wall if q < 0 else SIXTH

    for red, jobs in (
        (True, [(-3, "up", None)] + full(-2, -1) + [(0, "down", 1)]),
        (False, full(-2, -1, 0)),
        (True, [(-2, "up", None)] + full(-1, 0) + [(1, "down", 1)]),
        (False, full(-1, 0, 1)),
        (True, [(-1, "up", None)] + full(0, 1) + [(2, "down", 1)]),
    ):
        sweep_rows(red, jobs + mirror_jobs(jobs), odd, lane, get, factor)

    jobs = full(0, 1, 2)
    jobs = jobs + mirror_jobs(jobs)

    def tiles(i, carry):
        for u in range(4):
            t = i * 4 + u
            r = pl.multiple_of(t * 8 + 16, 8)
            rows = pl.ds(pl.multiple_of(t * 8, 8), 8)
            new = half_sweep(r, False, jobs, odd, lane, get, factor, rims=False)
            for q in range(Q):
                b = new[q][0] if q in new else bm[q, pl.ds(r, 8), :]
                v = rm[q, pl.ds(r, 8), :]
                at = mirrored(q, flip)
                obuf[at, 0, rows, :] = jnp.where(plain, b, v)
                obuf[at, 1, rows, :] = jnp.where(plain, v, b)
        return carry

    span = NY // OUT_CHUNKS
    copies = []
    for c in range(OUT_CHUNKS):
        lax.fori_loop(c * span // 32, (c + 1) * span // 32, tiles, 0)
        rows = pl.ds(c * span, span)
        copy = pltpu.make_async_copy(obuf.at[:, :, rows, :], out.at[:, :, rows, :], sems.at[c])
        copy.start()
        copies.append(copy)
    for copy in copies:
        copy.wait()


def smem():
    return pl.BlockSpec(memory_space=pltpu.SMEM)


def hbm():
    return pl.BlockSpec(memory_space=pl.ANY)


def near(value):
    return pltpu.with_memory_space_constraint(value, VM)


def room(mib):
    return pltpu.CompilerParams(vmem_limit_bytes=mib * 1024 * 1024)


def ring(size, step):
    return [(i, (i + step) % size) for i in range(size)]


def kernel(body, mib, outs, ins, **more):
    pairs = [i if isinstance(i, tuple) else (near(i), pl.BlockSpec(memory_space=VM)) for i in ins]
    arrays, specs = zip(*pairs)
    out_specs = more.pop("out_specs", [pl.BlockSpec(memory_space=VM)] * len(outs))
    return pl.pallas_call(
        body, out_shape=outs, in_specs=specs, out_specs=out_specs, compiler_params=room(mib), **more
    )(*arrays)


def send(value, axis, pairs):
    return lax.ppermute(near(value), axis, pairs)


def all_sweeps(field, source):
    gx = lax.axis_index("gx")
    last = lax.axis_size("gx") - 1
    walled = (gx == 0) | (gx == last)
    flip = (gx % 2 + 2 * walled.astype(jnp.int32))[None], smem()
    pairs = lax.axis_size("gx") // 2
    chip = [p for i in range(pairs) for p in ((2 * i, 2 * i + 1), (2 * i + 1, 2 * i))]
    across = [p for i in range(pairs - 1) for p in ((2 * i + 1, 2 * i + 2), (2 * i + 2, 2 * i + 1))]
    ny, nz = lax.axis_size("gy"), lax.axis_size("gz")

    blocks = [
        (pltpu.with_memory_space_constraint(a.reshape(Q, 2, NY, NZ), pltpu.HBM), hbm()) for a in (field, source)
    ]
    work, face, block = VM((Q, ROWS, NZ), F32), VM((Q, NY, NZ), F32), VM((Q, 2, NY, NZ), F32)
    rows, strip, corner = VM((NY, NZ), F32), VM((26, 8, NZ), F32), VM((50, 8, NZ), F32)

    bm, srm, sbm, zlow, zhigh = kernel(
        pack_kernel, 8, (work,) * 3 + (rows,) * 2, [flip] + blocks,
        scratch_shapes=[block, block, pltpu.SemaphoreType.DMA((2 * CHUNKS,))],
    )
    zr = send(zlow, "gz", ring(nz, -1))
    zl = send(zhigh, "gz", ring(nz, 1))
    high, low = kernel(face_kernel, 2, (face, face), [bm, srm, sbm])
    high = send(high, "gx", chip)
    low = send(low, "gx", across)
    ylow, yhigh = kernel(y_kernel, 2, (strip, strip), [bm, srm, sbm, zr, zl])
    yr = send(ylow, "gy", ring(ny, -1))
    yl = send(yhigh, "gy", ring(ny, 1))
    bh, srh, sbh = kernel(rim_kernel, 2, (work,) * 3, [zr, zl])
    chigh, clow, bm, srm, sbm, bh, srh, sbh = kernel(
        corner_kernel, 2, (corner, corner) + (work,) * 6, [yr, yl, zr, zl, bm, srm, sbm, bh, srh, sbh],
        input_output_aliases={4 + i: 2 + i for i in range(6)},
    )
    chigh = send(chigh, "gx", chip)
    clow = send(clow, "gx", across)
    bm, rm, bh, rh = kernel(
        inner_kernel, 4, (work,) * 4, [flip, bm, srm, sbm, bh, srh, sbh], input_output_aliases={1: 0, 4: 2}
    )
    halo3, halo2 = VM((6, ROWS, NZ), F32), VM((4, ROWS, NZ), F32)
    out = kernel(
        outer_kernel, 16, (jax.ShapeDtypeStruct((Q, 2, NY, NZ), F32),) + (work,) * 4,
        [flip, bm, rm, srm, sbm, bh, rh, srh, sbh, high, low, chigh, clow],
        out_specs=[hbm()] + [pl.BlockSpec(memory_space=VM)] * 4,
        input_output_aliases={1: 1, 2: 2, 5: 3, 6: 4},
        scratch_shapes=[halo3] * 6 + [halo2] * 2 + [block, pltpu.SemaphoreType.DMA((OUT_CHUNKS,))],
    )[0]
    return out.reshape(field.shape)


def solution(mesh):
    spec = P("gx", "gy", "gz")
    return jax.shard_map(all_sweeps, mesh=mesh, in_specs=(spec, spec), out_specs=spec, check_vma=False)
```

```python
import jax
import jax.numpy as jnp
from jax import lax
from jax.experimental import pallas as pl
from jax.experimental.pallas import tpu as pltpu
from jax.sharding import PartitionSpec as P


F32 = jnp.float32
VM = pltpu.VMEM
Q, NY, NZ = 8, 256, 128
ROWS = NY + 32
TILES = NY // 8
SIXTH = 1.0 / 6.0


def lanes_of():
    return lax.broadcasted_iota(jnp.int32, (8, 128), 1)


def odd_cells():
    return (lax.broadcasted_iota(jnp.int32, (8, 128), 0) + lanes_of()) % 2


def turn(value, shift):
    shift = shift % 128
    return value if shift == 0 else pltpu.roll(value, shift, 1)


def mirrored(q, flip):
    return q + flip * (Q - 1 - 2 * q)


BATCH = 80


def batched(count, size, body):
    def step(i, carry):
        body(i * size, size)
        return carry

    lax.fori_loop(0, count // size, step, 0)
    if count % size:
        body(count - count % size, count % size)


CHUNKS = 8


def segment(q):
    return q if q < 4 else 11 - q


def split_colours(fbuf, sbuf, at, rows, odd):
    f0, f1 = fbuf[at, 0, rows, :], fbuf[at, 1, rows, :]
    s0, s1 = sbuf[at, 0, rows, :], sbuf[at, 1, rows, :]
    return jnp.where(odd, f0, f1), jnp.where(odd, s1, s0), jnp.where(odd, s0, s1)


def pack_kernel(flip_ref, field, source, fbuf, sbuf, zlow, zhigh, sems):
    flip = flip_ref[0] % 2
    span = NY // CHUNKS
    copies = []
    for c in range(CHUNKS):
        rows = pl.ds(c * span, span)
        for n, (src, dst) in enumerate(((field, fbuf), (source, sbuf))):
            copy = pltpu.make_async_copy(src.at[:, :, rows, :], dst.at[:, :, rows, :], sems.at[2 * c + n])
            copy.start()
            copies.append(copy)
    odd = odd_cells() == 1
    lane = lanes_of()
    col = lane % 16
    left_half = lane < 64

    def tile(t):
        rows = pl.ds(pl.multiple_of(t * 8, 8), 8)
        acc = [jnp.zeros((8, 128), F32)] * 4
        for q in range(Q):
            b, sr, sb = split_colours(fbuf, sbuf, mirrored(q, flip), rows, odd)
            place = 16 * segment(q)
            here = lane // 16 == segment(q)
            parts = (
                turn(b, place),
                turn(jnp.where(left_half, sr, b), place + 6),
                turn(jnp.where(left_half, sb, sr), place + 11),
                turn(sb, place + 15),
            )
            acc = [jnp.where(here, new, old) for new, old in zip(parts, acc)]
        zlow[rows, :] = jnp.where(col < 6, acc[0], jnp.where(col < 11, acc[1], acc[2]))
        zhigh[rows, :] = jnp.where(col < 6, acc[1], jnp.where(col < 11, acc[2], acc[3]))

    for c in range(CHUNKS):
        copies[2 * c].wait()
        copies[2 * c + 1].wait()
        for u in range(span // 8):
            tile(c * span // 8 + u)


def face_kernel(flip_ref, fbuf, sbuf, bm, srm, sbm, high, low):
    flip = flip_ref[0] % 2
    odd = odd_cells() == 1

    def body(first, tiles):
        for u in range(tiles):
            r = pl.multiple_of((first + u) * 8, 8)
            rows = pl.ds(r, 8)
            put = pl.ds(pl.multiple_of(r + 16, 8), 8)
            for q in range(Q):
                values = split_colours(fbuf, sbuf, mirrored(q, flip), rows, odd)
                if q >= 4:
                    values = [turn(v, 64) for v in values]
                for ref, v in zip((bm, srm, sbm), values):
                    ref[q, put, :] = v
                out, d = (low, q) if q < 4 else (high, Q - 1 - q)
                if d < 3:
                    out[d, rows, :] = values[0]
                    out[3 + d, rows, :] = values[1]
                if d < 2:
                    out[6 + d, rows, :] = values[2]

    batched(TILES, 4, body)


def y_kernel(bm, srm, sbm, zr, zl, ylow, yhigh):
    for out, row in ((ylow, 0), (yhigh, NY - 8)):
        for n, ref in enumerate((bm, srm, sbm)):
            for q in range(Q):
                out[8 * n + q] = ref[q, row + 16:row + 24, :]
        out[24] = zr[row:row + 8, :]
        out[25] = zl[row:row + 8, :]


def put_rim(rows, r, l, place, refs):
    lane = lanes_of()
    col, half = lane % 16, lane % 64
    one = jnp.where(col < 6, l, r)
    two = jnp.where(col < 11, l, r)
    parts = [turn(r, -place), turn(one, -place - 6), turn(two, -place - 11), turn(l, -place - 15)]
    for n, (ref, width) in enumerate(zip(refs, (6, 5, 4))):
        ref[rows, :] = jnp.where(half < width, parts[n], jnp.where(half >= 64 - width, parts[n + 1], 0.0))


def rim_kernel(zr, zl, bh, srh, sbh):
    def body(first, tiles):
        for u in range(tiles):
            r = pl.multiple_of((first + u) * 8, 8)
            for a in range(4):
                refs = [ref.at[a] for ref in (bh, srh, sbh)]
                put_rim(pl.ds(pl.multiple_of(r + 16, 8), 8), zr[pl.ds(r, 8), :], zl[pl.ds(r, 8), :], 16 * a, refs)

    batched(TILES, 8, body)


def corner_kernel(yr, yl, zr, zl, bm_in, srm_in, sbm_in, bh_in, srh_in, sbh_in, high, low, bm, srm, sbm, bh, srh, sbh):
    del bm_in, srm_in, sbm_in, bh_in, srh_in, sbh_in
    lane = lanes_of()
    left_half = lane < 64
    for out, planes in ((low, (0, 1, 2)), (high, (7, 6, 5))):
        for side, ref in enumerate((yr, yl)):
            for d, q in enumerate(planes):
                out[8 * side + d] = ref[q]
                out[8 * side + 3 + d] = ref[8 + q]
                if d < 2:
                    out[8 * side + 6 + d] = ref[16 + q]

    def put(n, r, l):
        low[n] = jnp.where(left_half, r, turn(l, 64))
        high[n] = jnp.where(left_half, turn(r, 64), l)

    def body(first, tiles):
        for u in range(tiles):
            rows = pl.ds(pl.multiple_of((first + u) * 8, 8), 8)
            put(first + u + 17, zr[rows, :], zl[rows, :])

    put(16, yl[24], yl[25])
    put(49, yr[24], yr[25])
    batched(TILES, 16, body)
    for row, ref in ((8, yl), (NY + 16, yr)):
        for q in range(Q):
            bm[q, row:row + 8, :] = ref[q]
            srm[q, row:row + 8, :] = ref[8 + q]
            sbm[q, row:row + 8, :] = ref[16 + q]
        for a in range(4):
            put_rim(pl.ds(row, 8), ref[24], ref[25], 16 * a, [rim.at[a] for rim in (bh, srh, sbh)])


class Marks:
    def __init__(self, flip):
        self.lane = lanes_of()
        self.odd = (odd_cells() + flip) % 2 == 1
        turned = (self.lane >= 32) & (self.lane < 96)
        self.rim_odd = self.odd != turned
        self.turned = turned


def half_sweep(r, red, jobs, marks, main, rim, wall, rims=True):
    src, dst, add = ("black", "red", "sr") if red else ("red", "black", "sb")
    lane, odd, rim_odd = marks.lane, marks.odd, marks.rim_odd
    first, last, middle, before = lane == 0, lane == 127, lane == 64, lane == 63
    rows, above, below = pl.ds(r, 8), pl.ds(r - 1, 8), pl.ds(r + 1, 8)
    seen = {}

    def plane(q):
        if q not in seen:
            seen[q] = main(src, q)[rows, :]
        return seen[q]

    def edge(a):
        if ("rim", a) not in seen:
            seen["rim", a] = rim(src, a)[rows, :]
        return seen["rim", a]

    def pick(mark, up, down):
        return jnp.where(mark, up, down) if red else jnp.where(mark, down, up)

    done = {}
    for a, x, keep in jobs:
        b = Q - 1 - a
        turns = [(turn(v, 1), turn(v, 127)) for v in (plane(a), plane(b), edge(a))]
        (l0, r0), (l1, r1), (l2, r2) = turns
        beside = [
            jnp.where(first, l2, l0) + jnp.where(last, r2, r0),
            jnp.where(middle, l2, l1) + jnp.where(before, r2, r1),
        ]
        if rims:
            beside.append(
                jnp.where(first, l0, jnp.where(middle, l1, l2)) + jnp.where(last, r0, jnp.where(before, r1, r2))
            )
        inward = [lambda: plane(a + 1), lambda: plane(b - 1), lambda: edge(a + 1)]
        if a == 3:
            inward = [lambda: turn(plane(4), 64), lambda: turn(plane(3), 64), lambda: turn(edge(3), 64)]
        outward = [lambda: plane(a - 1), lambda: plane(b + 1), lambda: edge(a - 1)]
        refs = [main(src, a), main(src, b), rim(src, a)]
        adds = [main(add, a), main(add, b), rim(add, a)]
        olds = [main(dst, a), main(dst, b), rim(dst, a)]
        new = []
        for n in range(3 if rims else 2):
            if x == "up":
                along = inward[n]()
            elif x == "down":
                along = outward[n]()
            elif n == 1:
                along = pick(odd, outward[n](), inward[n]())
            else:
                along = pick(rim_odd if n == 2 else odd, inward[n](), outward[n]())
            total = (adds[n][rows, :] + (plane(a), plane(b), edge(a))[n]) + (along + beside[n])
            total = total + (refs[n][above, :] + refs[n][below, :])
            value = total * (SIXTH if a >= 0 else wall[n])
            if keep is not None:
                held = [odd, ~odd, rim_odd][n] if keep == 1 else [~odd, odd, ~rim_odd][n]
                value = jnp.where(held, olds[n][rows, :], value)
            new.append(value)
        done[a] = new
    return done


def sweep_rows(red, jobs, marks, main, rim, wall):
    dst = "red" if red else "black"

    def body(first, tiles):
        fresh = []
        for u in range(tiles):
            r = pl.multiple_of((first + u) * 8 + 8, 8)
            fresh.append((r, half_sweep(r, red, jobs, marks, main, rim, wall)))
        for r, done in fresh:
            for a, new in done.items():
                for ref, value in zip((main(dst, a), main(dst, Q - 1 - a), rim(dst, a)), new):
                    ref[pl.ds(r, 8), :] = value

    batched(TILES + 2, max(1, BATCH // len(jobs)), body)


def full(*planes):
    return [(a, "both", None) for a in planes]


def inner_kernel(flip_ref, bm_in, srm, sbm, bh_in, srh, sbh, bm, rm, bh, rh):
    del bm_in, bh_in
    marks = Marks(flip_ref[0] % 2)
    mains = {"black": bm, "red": rm, "sr": srm, "sb": sbm}
    edges = {"black": bh, "red": rh, "sr": srh, "sb": sbh}

    def main(kind, q):
        return mains[kind].at[q]

    def rim(kind, a):
        return edges[kind].at[a]

    for red, jobs in (
        (True, [(0, "up", None)] + full(1, 2, 3)),
        (False, full(1, 2, 3)),
        (True, [(1, "up", 0)] + full(2, 3)),
        (False, full(2, 3)),
        (True, [(2, "up", 0)] + full(3)),
        (False, full(3)),
    ):
        sweep_rows(red, jobs, marks, main, rim, None)


OUT_CHUNKS = 4


def outer_kernel(flip_ref, bm_in, rm_in, srm, sbm, bh_in, rh_in, srh, sbh, high, low, chigh, clow,
                 out, bm, rm, bh, rh, xbm, xbh, xrm, xrh, xsrm, xsrh, xsbm, xsbh, obuf, sems):
    del bm_in, rm_in, bh_in, rh_in
    flip = flip_ref[0] % 2
    marks = Marks(flip)
    lane = marks.lane
    outside = jnp.where(flip_ref[0] >= 2, 0.0, SIXTH)
    wall = (outside, SIXTH, jnp.where(marks.turned, SIXTH, outside))
    plain = odd_cells() == 1

    for side, face, corner in ((0, low, clow), (1, high, chigh)):
        for d in range(3):
            for n, (ref, deep) in enumerate(((xbm, 3), (xsrm, 3), (xsbm, 2))):
                if d < deep:
                    slot = deep * side + d
                    ref[slot, 8:16, :] = corner[8 + 3 * n + d]
                    ref[slot, 16:NY + 16, :] = face[3 * n + d]
                    ref[slot, NY + 16:NY + 24, :] = corner[3 * n + d]

    def fill(first, tiles):
        for u in range(tiles):
            t = first + u
            rows = pl.ds(pl.multiple_of(t * 8 + 8, 8), 8)
            one = clow[16 + t]
            two = turn(chigh[16 + t], 64)
            r = jnp.where(lane < 64, one, two)
            l = turn(jnp.where(lane < 64, two, one), 64)
            for d in range(3):
                put_rim(rows, r, l, 16 * d, [ref.at[d] for ref in (xbh, xsrh, xsbh)[:3 if d < 2 else 2]])

    batched(TILES + 2, 8, fill)

    mains = {"black": (bm, xbm), "red": (rm, xrm), "sr": (srm, xsrm), "sb": (sbm, xsbm)}
    edges = {"black": (bh, xbh), "red": (rh, xrh), "sr": (srh, xsrh), "sb": (sbh, xsbh)}

    def main(kind, q):
        own, halo = mains[kind]
        if 0 <= q < Q:
            return own.at[q]
        return halo.at[-1 - q if q < 0 else (2 if kind == "sb" else 3) + q - Q]

    def rim(kind, a):
        own, halo = edges[kind]
        return own.at[a] if a >= 0 else halo.at[-1 - a]

    for red, jobs in (
        (True, [(-3, "up", None)] + full(-2, -1) + [(0, "down", 1)]),
        (False, full(-2, -1, 0)),
        (True, [(-2, "up", None)] + full(-1, 0) + [(1, "down", 1)]),
        (False, full(-1, 0, 1)),
        (True, [(-1, "up", None)] + full(0, 1) + [(2, "down", 1)]),
    ):
        sweep_rows(red, jobs, marks, main, rim, wall)

    def tiles(i, carry):
        done = []
        for u in range(8):
            t = i * 8 + u
            r = pl.multiple_of(t * 8 + 16, 8)
            done.append((t, r, half_sweep(r, False, full(0, 1, 2), marks, main, rim, wall, rims=False)))
        for t, r, new in done:
            rows = pl.ds(pl.multiple_of(t * 8, 8), 8)
            for q in range(Q):
                a = min(q, Q - 1 - q)
                b = new[a][0 if q == a else 1] if a in new else bm[q, pl.ds(r, 8), :]
                v = rm[q, pl.ds(r, 8), :]
                at = mirrored(q, flip)
                for n, value in enumerate((jnp.where(plain, b, v), jnp.where(plain, v, b))):
                    obuf[at, n, rows, :] = value if q < 4 else turn(value, 64)
        return carry

    span = NY // OUT_CHUNKS
    copies = []
    for c in range(OUT_CHUNKS):
        lax.fori_loop(c * span // 64, (c + 1) * span // 64, tiles, 0)
        rows = pl.ds(c * span, span)
        copy = pltpu.make_async_copy(obuf.at[:, :, rows, :], out.at[:, :, rows, :], sems.at[c])
        copy.start()
        copies.append(copy)
    for copy in copies:
        copy.wait()


def smem():
    return pl.BlockSpec(memory_space=pltpu.SMEM)


def hbm():
    return pl.BlockSpec(memory_space=pl.ANY)


def near(value):
    return pltpu.with_memory_space_constraint(value, VM)


def room(mib):
    return pltpu.CompilerParams(vmem_limit_bytes=mib * 1024 * 1024)


def ring(size, step):
    return [(i, (i + step) % size) for i in range(size)]


def kernel(body, mib, outs, ins, **more):
    pairs = [i if isinstance(i, tuple) else (near(i), pl.BlockSpec(memory_space=VM)) for i in ins]
    arrays, specs = zip(*pairs)
    out_specs = more.pop("out_specs", [pl.BlockSpec(memory_space=VM)] * len(outs))
    return pl.pallas_call(
        body, out_shape=outs, in_specs=specs, out_specs=out_specs, compiler_params=room(mib), **more
    )(*arrays)


def send(value, axis, pairs):
    return lax.ppermute(near(value), axis, pairs)


def all_sweeps(field, source):
    gx = lax.axis_index("gx")
    last = lax.axis_size("gx") - 1
    walled = (gx == 0) | (gx == last)
    flip = (gx % 2 + 2 * walled.astype(jnp.int32))[None], smem()
    pairs = lax.axis_size("gx") // 2
    chip = [p for i in range(pairs) for p in ((2 * i, 2 * i + 1), (2 * i + 1, 2 * i))]
    across = [p for i in range(pairs - 1) for p in ((2 * i + 1, 2 * i + 2), (2 * i + 2, 2 * i + 1))]
    ny, nz = lax.axis_size("gy"), lax.axis_size("gz")

    blocks = [
        (pltpu.with_memory_space_constraint(a.reshape(Q, 2, NY, NZ), pltpu.HBM), hbm()) for a in (field, source)
    ]
    edge = VM((4, ROWS, NZ), F32)
    work, face, block = VM((Q, ROWS, NZ), F32), VM((Q, NY, NZ), F32), VM((Q, 2, NY, NZ), F32)
    rows, strip, corner = VM((NY, NZ), F32), VM((26, 8, NZ), F32), VM((50, 8, NZ), F32)

    fbuf, sbuf, zlow, zhigh = kernel(
        pack_kernel, 2, (block, block, rows, rows), [flip] + blocks,
        scratch_shapes=[pltpu.SemaphoreType.DMA((2 * CHUNKS,))],
    )
    zr = send(zlow, "gz", ring(nz, -1))
    zl = send(zhigh, "gz", ring(nz, 1))
    bm, srm, sbm, high, low = kernel(face_kernel, 2, (work,) * 3 + (face,) * 2, [flip, fbuf, sbuf])
    high = send(high, "gx", chip)
    low = send(low, "gx", across)
    ylow, yhigh = kernel(y_kernel, 2, (strip, strip), [bm, srm, sbm, zr, zl])
    yr = send(ylow, "gy", ring(ny, -1))
    yl = send(yhigh, "gy", ring(ny, 1))
    bh, srh, sbh = kernel(rim_kernel, 2, (edge,) * 3, [zr, zl])
    chigh, clow, bm, srm, sbm, bh, srh, sbh = kernel(
        corner_kernel, 2, (corner, corner) + (work,) * 3 + (edge,) * 3, [yr, yl, zr, zl, bm, srm, sbm, bh, srh, sbh],
        input_output_aliases={4 + i: 2 + i for i in range(6)},
    )
    chigh = send(chigh, "gx", chip)
    clow = send(clow, "gx", across)
    bm, rm, bh, rh = kernel(
        inner_kernel, 4, (work, work, edge, edge), [flip, bm, srm, sbm, bh, srh, sbh], input_output_aliases={1: 0, 4: 2}
    )
    halo = [VM((n, ROWS, NZ), F32) for n in (6, 3, 6, 3, 6, 3, 4, 2)]
    out = kernel(
        outer_kernel, 16, (jax.ShapeDtypeStruct((Q, 2, NY, NZ), F32), work, work, edge, edge),
        [flip, bm, rm, srm, sbm, bh, rh, srh, sbh, high, low, chigh, clow],
        out_specs=[hbm()] + [pl.BlockSpec(memory_space=VM)] * 4,
        input_output_aliases={1: 1, 2: 2, 5: 3, 6: 4},
        scratch_shapes=halo + [block, pltpu.SemaphoreType.DMA((OUT_CHUNKS,))],
    )[0]
    return out.reshape(field.shape)


def solution(mesh):
    spec = P("gx", "gy", "gz")
    return jax.shard_map(all_sweeps, mesh=mesh, in_specs=(spec, spec), out_specs=spec, check_vma=False)
```

```python
import jax
import jax.numpy as jnp
from jax import lax
from jax.experimental import pallas as pl
from jax.experimental.pallas import tpu as pltpu
from jax.sharding import PartitionSpec as P


F32 = jnp.float32
VM = pltpu.VMEM
Q, NY, NZ = 8, 256, 128
ROWS = NY + 32
TILES = NY // 8
SIXTH = 1.0 / 6.0


def lanes_of():
    return lax.broadcasted_iota(jnp.int32, (8, 128), 1)


def odd_cells():
    return (lax.broadcasted_iota(jnp.int32, (8, 128), 0) + lanes_of()) % 2


def turn(value, shift):
    shift = shift % 128
    return value if shift == 0 else pltpu.roll(value, shift, 1)


def mirrored(q, flip):
    return q + flip * (Q - 1 - 2 * q)


BATCH = 80


def batched(count, size, body):
    def step(i, carry):
        body(i * size, size)
        return carry

    lax.fori_loop(0, count // size, step, 0)
    if count % size:
        body(count - count % size, count % size)


CHUNKS = 8


def segment(q):
    return q if q < 4 else 11 - q


def split_colours(fbuf, sbuf, at, rows, odd):
    f0, f1 = fbuf[at, 0, rows, :], fbuf[at, 1, rows, :]
    s0, s1 = sbuf[at, 0, rows, :], sbuf[at, 1, rows, :]
    return jnp.where(odd, f0, f1), jnp.where(odd, s1, s0), jnp.where(odd, s0, s1)


def pack_kernel(flip_ref, field, source, fbuf, sbuf, zlow, zhigh, sems):
    flip = flip_ref[0] % 2
    span = NY // CHUNKS
    copies = []
    for c in range(CHUNKS):
        rows = pl.ds(c * span, span)
        for n, (src, dst) in enumerate(((field, fbuf), (source, sbuf))):
            copy = pltpu.make_async_copy(src.at[:, :, rows, :], dst.at[:, :, rows, :], sems.at[2 * c + n])
            copy.start()
            copies.append(copy)
    odd = odd_cells() == 1
    lane = lanes_of()
    col = lane % 16
    left_half = lane < 64

    def tile(t):
        rows = pl.ds(pl.multiple_of(t * 8, 8), 8)
        acc = [jnp.zeros((8, 128), F32)] * 3
        for q in range(Q):
            b, sr, sb = split_colours(fbuf, sbuf, mirrored(q, flip), rows, odd)
            place = 16 * segment(q)
            here = lane // 16 == segment(q)
            near_here = (lane + 4) % 128 // 16 == segment(q)
            acc[0] = jnp.where(near_here, turn(jnp.where(left_half, b, sb), place), acc[0])
            acc[1] = jnp.where(here, turn(jnp.where(left_half, sr, b), place + 6), acc[1])
            acc[2] = jnp.where(here, turn(jnp.where(left_half, sb, sr), place + 11), acc[2])
        zlow[rows, :] = jnp.where(col < 6, acc[0], jnp.where(col < 11, acc[1], acc[2]))
        zhigh[rows, :] = jnp.where(col < 6, acc[1], jnp.where(col < 12, acc[2], acc[0]))

    for c in range(CHUNKS):
        copies[2 * c].wait()
        copies[2 * c + 1].wait()
        for u in range(span // 8):
            tile(c * span // 8 + u)


def face_kernel(flip_ref, fbuf, sbuf, bm, srm, sbm, high, low):
    flip = flip_ref[0] % 2
    odd = odd_cells() == 1

    def body(first, tiles):
        for u in range(tiles):
            r = pl.multiple_of((first + u) * 8, 8)
            rows = pl.ds(r, 8)
            put = pl.ds(pl.multiple_of(r + 16, 8), 8)
            for q in range(Q):
                values = split_colours(fbuf, sbuf, mirrored(q, flip), rows, odd)
                if q >= 4:
                    values = [turn(v, 64) for v in values]
                for ref, v in zip((bm, srm, sbm), values):
                    ref[q, put, :] = v
                out, d = (low, q) if q < 4 else (high, Q - 1 - q)
                if d < 3:
                    out[d, rows, :] = values[0]
                    out[3 + d, rows, :] = values[1]
                if d < 2:
                    out[6 + d, rows, :] = values[2]

    batched(TILES, 4, body)


def y_kernel(bm, srm, sbm, zr, zl, ylow, yhigh):
    for out, row in ((ylow, 0), (yhigh, NY - 8)):
        for n, ref in enumerate((bm, srm, sbm)):
            for q in range(Q):
                out[8 * n + q] = ref[q, row + 16:row + 24, :]
        out[24] = zr[row:row + 8, :]
        out[25] = zl[row:row + 8, :]


def put_rim(rows, r, l, place, refs):
    lane = lanes_of()
    col, half = lane % 16, lane % 64
    parts = [
        turn(jnp.where(col < 12, r, l), -place),
        turn(jnp.where(col < 6, l, r), -place - 6),
        turn(jnp.where(col < 11, l, r), -place - 11),
    ]
    for n, (ref, width) in enumerate(zip(refs, (6, 5, 4))):
        ref[rows, :] = jnp.where(half < width, parts[n], jnp.where(half >= 64 - width, parts[(n + 1) % 3], 0.0))


def edges_low(r, l):
    return jnp.where(lanes_of() < 60, r, turn(l, 64))


def edges_high(r, l):
    return jnp.where(lanes_of() < 60, turn(r, 64), l)


def put_halo_rims(rows, low, high, refs):
    lane = lanes_of()
    high = turn(high, 64)
    r = jnp.where(lane < 60, low, high)
    l = turn(jnp.where((lane >= 60) & (lane < 124), low, high), 64)
    for d in range(3):
        put_rim(rows, r, l, 16 * d, [ref.at[d] for ref in refs[:3 if d < 2 else 2]])


def edge_kernel(after, zr, zl, high, low):
    del after

    def body(first, tiles):
        for u in range(tiles):
            rows = pl.ds(pl.multiple_of((first + u) * 8, 8), 8)
            low[rows, :] = edges_low(zr[rows, :], zl[rows, :])
            high[rows, :] = edges_high(zr[rows, :], zl[rows, :])

    batched(TILES, 16, body)


def corner_kernel(yr, yl, bm_in, srm_in, sbm_in, bh_in, srh_in, sbh_in, high, low, bm, srm, sbm, bh, srh, sbh):
    del bm_in, srm_in, sbm_in, bh_in, srh_in, sbh_in
    for out, planes, pack in ((low, (0, 1, 2), edges_low), (high, (7, 6, 5), edges_high)):
        for side, ref in enumerate((yr, yl)):
            for d, q in enumerate(planes):
                out[8 * side + d] = ref[q]
                out[8 * side + 3 + d] = ref[8 + q]
                if d < 2:
                    out[8 * side + 6 + d] = ref[16 + q]
            out[16 + side] = pack(ref[24], ref[25])
    for row, ref in ((8, yl), (NY + 16, yr)):
        for q in range(Q):
            bm[q, row:row + 8, :] = ref[q]
            srm[q, row:row + 8, :] = ref[8 + q]
            sbm[q, row:row + 8, :] = ref[16 + q]
        for a in range(4):
            put_rim(pl.ds(row, 8), ref[24], ref[25], 16 * a, [rim.at[a] for rim in (bh, srh, sbh)])


class Marks:
    def __init__(self, flip):
        self.lane = lanes_of()
        self.odd = (odd_cells() + flip) % 2 == 1
        turned = (self.lane >= 32) & (self.lane < 96)
        self.rim_odd = self.odd != turned
        self.turned = turned


def half_sweep(r, red, jobs, marks, main, rim, wall, rims=True):
    src, dst, add = ("black", "red", "sr") if red else ("red", "black", "sb")
    lane, odd, rim_odd = marks.lane, marks.odd, marks.rim_odd
    first, last, middle, before = lane == 0, lane == 127, lane == 64, lane == 63
    rows, above, below = pl.ds(r, 8), pl.ds(r - 1, 8), pl.ds(r + 1, 8)
    seen = {}

    def plane(q):
        if q not in seen:
            seen[q] = main(src, q)[rows, :]
        return seen[q]

    def edge(a):
        if ("rim", a) not in seen:
            seen["rim", a] = rim(src, a)[rows, :]
        return seen["rim", a]

    def pick(mark, up, down):
        return jnp.where(mark, up, down) if red else jnp.where(mark, down, up)

    done = {}
    for a, x, keep in jobs:
        b = Q - 1 - a
        turns = [(turn(v, 1), turn(v, 127)) for v in (plane(a), plane(b), edge(a))]
        (l0, r0), (l1, r1), (l2, r2) = turns
        beside = [
            jnp.where(first, l2, l0) + jnp.where(last, r2, r0),
            jnp.where(middle, l2, l1) + jnp.where(before, r2, r1),
        ]
        if rims:
            beside.append(
                jnp.where(first, l0, jnp.where(middle, l1, l2)) + jnp.where(last, r0, jnp.where(before, r1, r2))
            )
        inward = [lambda: plane(a + 1), lambda: plane(b - 1), lambda: edge(a + 1)]
        if a == 3:
            inward = [lambda: turn(plane(4), 64), lambda: turn(plane(3), 64), lambda: turn(edge(3), 64)]
        outward = [lambda: plane(a - 1), lambda: plane(b + 1), lambda: edge(a - 1)]
        refs = [main(src, a), main(src, b), rim(src, a)]
        adds = [main(add, a), main(add, b), rim(add, a)]
        olds = [main(dst, a), main(dst, b), rim(dst, a)]
        new = []
        for n in range(3 if rims else 2):
            if x == "up":
                along = inward[n]()
            elif x == "down":
                along = outward[n]()
            elif n == 1:
                along = pick(odd, outward[n](), inward[n]())
            else:
                along = pick(rim_odd if n == 2 else odd, inward[n](), outward[n]())
            total = (adds[n][rows, :] + (plane(a), plane(b), edge(a))[n]) + (along + beside[n])
            total = total + (refs[n][above, :] + refs[n][below, :])
            value = total * (SIXTH if a >= 0 else wall[n])
            if keep is not None:
                held = [odd, ~odd, rim_odd][n] if keep == 1 else [~odd, odd, ~rim_odd][n]
                value = jnp.where(held, olds[n][rows, :], value)
            new.append(value)
        done[a] = new
    return done


EVERY = ((0, TILES + 2),)


def sweep_rows(red, jobs, marks, main, rim, wall, spans=EVERY):
    dst = "red" if red else "black"

    def body(first, tiles):
        fresh = []
        for u in range(tiles):
            r = pl.multiple_of((first + u) * 8 + 8, 8)
            fresh.append((r, half_sweep(r, red, jobs, marks, main, rim, wall)))
        for r, done in fresh:
            for a, new in done.items():
                for ref, value in zip((main(dst, a), main(dst, Q - 1 - a), rim(dst, a)), new):
                    ref[pl.ds(r, 8), :] = value

    for start, count in spans:
        batched(count, max(1, BATCH // len(jobs)), lambda first, tiles: body(start + first, tiles))


def full(*planes):
    return [(a, "both", None) for a in planes]


INNER = (
    (True, [(0, "up", None)] + full(1, 2, 3)),
    (False, full(1, 2, 3)),
    (True, [(1, "up", 0)] + full(2, 3)),
    (False, full(2, 3)),
    (True, [(2, "up", 0)] + full(3)),
    (False, full(3)),
)
EARLY = 2


def lookups(mains, edges):
    def main(kind, q):
        return mains[kind].at[q]

    def rim(kind, a):
        return edges[kind].at[a]

    return main, rim


def early_kernel(flip_ref, after, zr, zl, bm_in, srm, sbm, bm, rm, bh, rh, srh, sbh):
    del after, bm_in
    marks = Marks(flip_ref[0] % 2)

    def body(first, tiles):
        for u in range(tiles):
            r = pl.multiple_of((first + u) * 8, 8)
            for a in range(4):
                refs = [ref.at[a] for ref in (bh, srh, sbh)]
                put_rim(pl.ds(pl.multiple_of(r + 16, 8), 8), zr[pl.ds(r, 8), :], zl[pl.ds(r, 8), :], 16 * a, refs)

    batched(TILES, 8, body)
    main, rim = lookups({"black": bm, "red": rm, "sr": srm, "sb": sbm}, {"black": bh, "red": rh, "sr": srh, "sb": sbh})
    for n, (red, jobs) in enumerate(INNER[:EARLY]):
        sweep_rows(red, jobs, marks, main, rim, None, ((2 + n, TILES - 2 - 2 * n),))


def inner_kernel(flip_ref, bm_in, rm_in, srm, sbm, bh_in, rh_in, srh, sbh, bm, rm, bh, rh):
    del bm_in, rm_in, bh_in, rh_in
    marks = Marks(flip_ref[0] % 2)
    main, rim = lookups({"black": bm, "red": rm, "sr": srm, "sb": sbm}, {"black": bh, "red": rh, "sr": srh, "sb": sbh})
    for n, (red, jobs) in enumerate(INNER):
        spans = ((0, 2 + n), (TILES - n, 2 + n)) if n < EARLY else EVERY
        sweep_rows(red, jobs, marks, main, rim, None, spans)


def halo_kernel(after, high, low, ehigh, elow, xbm, xsrm, xsbm, xbh, xsrh, xsbh):
    del after

    def body(first, tiles):
        for u in range(tiles):
            r = pl.multiple_of((first + u) * 8, 8)
            rows, put = pl.ds(r, 8), pl.ds(pl.multiple_of(r + 16, 8), 8)
            for side, face in enumerate((low, high)):
                for d in range(3):
                    xbm[3 * side + d, put, :] = face[d, rows, :]
                    xsrm[3 * side + d, put, :] = face[3 + d, rows, :]
                    if d < 2:
                        xsbm[2 * side + d, put, :] = face[6 + d, rows, :]
            put_halo_rims(put, elow[rows, :], ehigh[rows, :], (xbh, xsrh, xsbh))

    batched(TILES, 8, body)


OUT_CHUNKS = 4


def outer_kernel(flip_ref, bm_in, rm_in, srm, sbm, bh_in, rh_in, srh, sbh, chigh, clow,
                 xbm_in, xsrm_in, xsbm_in, xbh_in, xsrh_in, xsbh_in,
                 out, bm, rm, bh, rh, xbm, xsrm, xsbm, xbh, xsrh, xsbh, xrm, xrh, obuf, sems):
    del bm_in, rm_in, bh_in, rh_in, xbm_in, xsrm_in, xsbm_in, xbh_in, xsrh_in, xsbh_in
    flip = flip_ref[0] % 2
    marks = Marks(flip)
    outside = jnp.where(flip_ref[0] >= 2, 0.0, SIXTH)
    wall = (outside, SIXTH, jnp.where(marks.turned, SIXTH, outside))
    plain = odd_cells() == 1

    for y, (row, n) in enumerate(((NY + 16, 0), (8, 8))):
        for side, corner in enumerate((clow, chigh)):
            for d in range(3):
                xbm[3 * side + d, row:row + 8, :] = corner[n + d]
                xsrm[3 * side + d, row:row + 8, :] = corner[n + 3 + d]
                if d < 2:
                    xsbm[2 * side + d, row:row + 8, :] = corner[n + 6 + d]
        put_halo_rims(pl.ds(row, 8), clow[16 + y], chigh[16 + y], (xbh, xsrh, xsbh))

    mains = {"black": (bm, xbm), "red": (rm, xrm), "sr": (srm, xsrm), "sb": (sbm, xsbm)}
    edges = {"black": (bh, xbh), "red": (rh, xrh), "sr": (srh, xsrh), "sb": (sbh, xsbh)}

    def main(kind, q):
        own, halo = mains[kind]
        if 0 <= q < Q:
            return own.at[q]
        return halo.at[-1 - q if q < 0 else (2 if kind == "sb" else 3) + q - Q]

    def rim(kind, a):
        own, halo = edges[kind]
        return own.at[a] if a >= 0 else halo.at[-1 - a]

    for red, jobs in (
        (True, [(-3, "up", None)] + full(-2, -1) + [(0, "down", 1)]),
        (False, full(-2, -1, 0)),
        (True, [(-2, "up", None)] + full(-1, 0) + [(1, "down", 1)]),
        (False, full(-1, 0, 1)),
        (True, [(-1, "up", None)] + full(0, 1) + [(2, "down", 1)]),
    ):
        sweep_rows(red, jobs, marks, main, rim, wall)

    def tiles(i, carry):
        done = []
        for u in range(8):
            t = i * 8 + u
            r = pl.multiple_of(t * 8 + 16, 8)
            done.append((t, r, half_sweep(r, False, full(0, 1, 2), marks, main, rim, wall, rims=False)))
        for t, r, new in done:
            rows = pl.ds(pl.multiple_of(t * 8, 8), 8)
            for q in range(Q):
                a = min(q, Q - 1 - q)
                b = new[a][0 if q == a else 1] if a in new else bm[q, pl.ds(r, 8), :]
                v = rm[q, pl.ds(r, 8), :]
                at = mirrored(q, flip)
                for n, value in enumerate((jnp.where(plain, b, v), jnp.where(plain, v, b))):
                    obuf[at, n, rows, :] = value if q < 4 else turn(value, 64)
        return carry

    span = NY // OUT_CHUNKS
    copies = []
    for c in range(OUT_CHUNKS):
        lax.fori_loop(c * span // 64, (c + 1) * span // 64, tiles, 0)
        rows = pl.ds(c * span, span)
        copy = pltpu.make_async_copy(obuf.at[:, :, rows, :], out.at[:, :, rows, :], sems.at[c])
        copy.start()
        copies.append(copy)
    for copy in copies:
        copy.wait()


def smem():
    return pl.BlockSpec(memory_space=pltpu.SMEM)


def hbm():
    return pl.BlockSpec(memory_space=pl.ANY)


def near(value):
    return pltpu.with_memory_space_constraint(value, VM)


def room(mib):
    return pltpu.CompilerParams(vmem_limit_bytes=mib * 1024 * 1024)


def ring(size, step):
    return [(i, (i + step) % size) for i in range(size)]


def kernel(body, mib, outs, ins, **more):
    pairs = [i if isinstance(i, tuple) else (near(i), pl.BlockSpec(memory_space=VM)) for i in ins]
    arrays, specs = zip(*pairs)
    out_specs = more.pop("out_specs", [pl.BlockSpec(memory_space=VM)] * len(outs))
    return pl.pallas_call(
        body, out_shape=outs, in_specs=specs, out_specs=out_specs, compiler_params=room(mib), **more
    )(*arrays)


def send(value, axis, pairs):
    return lax.ppermute(near(value), axis, pairs)


def all_sweeps(field, source):
    gx = lax.axis_index("gx")
    last = lax.axis_size("gx") - 1
    walled = (gx == 0) | (gx == last)
    flip = (gx % 2 + 2 * walled.astype(jnp.int32))[None], smem()
    pairs = lax.axis_size("gx") // 2
    chip = [p for i in range(pairs) for p in ((2 * i, 2 * i + 1), (2 * i + 1, 2 * i))]
    across = [p for i in range(pairs - 1) for p in ((2 * i + 1, 2 * i + 2), (2 * i + 2, 2 * i + 1))]
    ny, nz = lax.axis_size("gy"), lax.axis_size("gz")

    blocks = [
        (pltpu.with_memory_space_constraint(a.reshape(Q, 2, NY, NZ), pltpu.HBM), hbm()) for a in (field, source)
    ]
    edge = VM((4, ROWS, NZ), F32)
    work, face, block = VM((Q, ROWS, NZ), F32), VM((Q, NY, NZ), F32), VM((Q, 2, NY, NZ), F32)
    rows, strip, corner = VM((NY, NZ), F32), VM((26, 8, NZ), F32), VM((18, 8, NZ), F32)

    fbuf, sbuf, zlow, zhigh = kernel(
        pack_kernel, 2, (block, block, rows, rows), [flip] + blocks,
        scratch_shapes=[pltpu.SemaphoreType.DMA((2 * CHUNKS,))],
    )
    zr = send(zlow, "gz", ring(nz, -1))
    zl = send(zhigh, "gz", ring(nz, 1))
    bm, srm, sbm, high, low = kernel(face_kernel, 2, (work,) * 3 + (face,) * 2, [flip, fbuf, sbuf])
    high = send(high, "gx", chip)
    low = send(low, "gx", across)
    ylow, yhigh = kernel(y_kernel, 2, (strip, strip), [bm, srm, sbm, zr, zl])
    yr = send(ylow, "gy", ring(ny, -1))
    yl = send(yhigh, "gy", ring(ny, 1))
    ehigh, elow = kernel(edge_kernel, 2, (rows, rows), [(ylow, hbm()), zr, zl])
    ehigh = send(ehigh, "gx", chip)
    elow = send(elow, "gx", across)
    bm, rm, bh, rh, srh, sbh = kernel(
        early_kernel, 4, (work, work) + (edge,) * 4, [flip, (ylow, hbm()), zr, zl, bm, srm, sbm],
        input_output_aliases={4: 0},
    )
    chigh, clow, bm, srm, sbm, bh, srh, sbh = kernel(
        corner_kernel, 2, (corner, corner) + (work,) * 3 + (edge,) * 3, [yr, yl, bm, srm, sbm, bh, srh, sbh],
        input_output_aliases={2 + i: 2 + i for i in range(6)},
    )
    turn_of_halo = clow
    chigh = send(chigh, "gx", chip)
    clow = send(clow, "gx", across)
    bm, rm, bh, rh = kernel(
        inner_kernel, 4, (work, work, edge, edge), [flip, bm, rm, srm, sbm, bh, rh, srh, sbh],
        input_output_aliases={1: 0, 2: 1, 5: 2, 6: 3},
    )
    halo = [VM((n, ROWS, NZ), F32) for n in (6, 6, 4, 3, 3, 2)]
    halos = kernel(halo_kernel, 2, halo, [(turn_of_halo, hbm()), high, low, ehigh, elow])
    out = kernel(
        outer_kernel, 12,
        [jax.ShapeDtypeStruct((Q, 2, NY, NZ), F32), work, work, edge, edge] + halo,
        [flip, bm, rm, srm, sbm, bh, rh, srh, sbh, chigh, clow, *halos],
        out_specs=[hbm()] + [pl.BlockSpec(memory_space=VM)] * 10,
        input_output_aliases={1: 1, 2: 2, 5: 3, 6: 4, **{11 + i: 5 + i for i in range(6)}},
        scratch_shapes=[halo[0], halo[3], block, pltpu.SemaphoreType.DMA((OUT_CHUNKS,))],
    )[0]
    return out.reshape(field.shape)


def solution(mesh):
    spec = P("gx", "gy", "gz")
    return jax.shard_map(all_sweeps, mesh=mesh, in_specs=(spec, spec), out_specs=spec, check_vma=False)
```

```python
import jax
import jax.numpy as jnp
from jax import lax
from jax.experimental import pallas as pl
from jax.experimental.pallas import tpu as pltpu
from jax.sharding import PartitionSpec as P


F32 = jnp.float32
VM = pltpu.VMEM
Q, NY, NZ = 8, 256, 128
ROWS = NY + 32
TILES = NY // 8
SIXTH = 1.0 / 6.0


def lanes_of():
    return lax.broadcasted_iota(jnp.int32, (8, 128), 1)


def odd_cells():
    return (lax.broadcasted_iota(jnp.int32, (8, 128), 0) + lanes_of()) % 2


def turn(value, shift):
    shift = shift % 128
    return value if shift == 0 else pltpu.roll(value, shift, 1)


def mirrored(q, flip):
    return q + flip * (Q - 1 - 2 * q)


BATCH = 80


def batched(count, size, body):
    def step(i, carry):
        body(i * size, size)
        return carry

    lax.fori_loop(0, count // size, step, 0)
    if count % size:
        body(count - count % size, count % size)


CHUNKS = 8


def segment(q):
    return q if q < 4 else 11 - q


def split_colours(fbuf, sbuf, at, rows, odd):
    f0, f1 = fbuf[at, 0, rows, :], fbuf[at, 1, rows, :]
    s0, s1 = sbuf[at, 0, rows, :], sbuf[at, 1, rows, :]
    return jnp.where(odd, f0, f1), jnp.where(odd, s1, s0), jnp.where(odd, s0, s1)


def pack_kernel(flip_ref, field, source, fbuf, sbuf, zlow, zhigh, sems):
    flip = flip_ref[0] % 2
    span = NY // CHUNKS
    copies = []
    for c in range(CHUNKS):
        rows = pl.ds(c * span, span)
        for n, (src, dst) in enumerate(((field, fbuf), (source, sbuf))):
            copy = pltpu.make_async_copy(src.at[:, :, rows, :], dst.at[:, :, rows, :], sems.at[2 * c + n])
            copy.start()
            copies.append(copy)
    odd = odd_cells() == 1
    lane = lanes_of()
    col = lane % 16
    left_half = lane < 64

    def tile(t):
        rows = pl.ds(pl.multiple_of(t * 8, 8), 8)
        acc = [jnp.zeros((8, 128), F32)] * 3
        for q in range(Q):
            b, sr, sb = split_colours(fbuf, sbuf, mirrored(q, flip), rows, odd)
            place = 16 * segment(q)
            here = lane // 16 == segment(q)
            near_here = (lane + 4) % 128 // 16 == segment(q)
            acc[0] = jnp.where(near_here, turn(jnp.where(left_half, b, sb), place), acc[0])
            acc[1] = jnp.where(here, turn(jnp.where(left_half, sr, b), place + 6), acc[1])
            acc[2] = jnp.where(here, turn(jnp.where(left_half, sb, sr), place + 11), acc[2])
        zlow[rows, :] = jnp.where(col < 6, acc[0], jnp.where(col < 11, acc[1], acc[2]))
        zhigh[rows, :] = jnp.where(col < 6, acc[1], jnp.where(col < 12, acc[2], acc[0]))

    for c in range(CHUNKS):
        copies[2 * c].wait()
        copies[2 * c + 1].wait()
        for u in range(span // 8):
            tile(c * span // 8 + u)


def face_kernel(flip_ref, fbuf, sbuf, bm, srm, sbm, high, low):
    flip = flip_ref[0] % 2
    odd = odd_cells() == 1

    def body(first, tiles):
        for u in range(tiles):
            r = pl.multiple_of((first + u) * 8, 8)
            rows = pl.ds(r, 8)
            put = pl.ds(pl.multiple_of(r + 16, 8), 8)
            for q in range(Q):
                values = split_colours(fbuf, sbuf, mirrored(q, flip), rows, odd)
                if q >= 4:
                    values = [turn(v, 64) for v in values]
                for ref, v in zip((bm, srm, sbm), values):
                    ref[q, put, :] = v
                out, d = (low, q) if q < 4 else (high, Q - 1 - q)
                if d < 3:
                    out[d, put, :] = values[0]
                    out[3 + d, put, :] = values[1]
                if d < 2:
                    out[6 + d, put, :] = values[2]

    batched(TILES, 4, body)


def rows_of():
    return lax.broadcasted_iota(jnp.int32, (8, 128), 0)


def pack_low(b, sr, sb):
    row = rows_of()
    return jnp.where(row < 6, b, pltpu.roll(sr, 3, 0)), jnp.where(row < 4, sb, pltpu.roll(sr, 4, 0))


def unpack_low(one, two):
    return one, jnp.where(rows_of() < 3, pltpu.roll(two, 4, 0), pltpu.roll(one, 5, 0)), two


def pack_high(b, sr, sb):
    row = rows_of()
    return jnp.where(row >= 2, b, pltpu.roll(sr, 5, 0)), jnp.where(row >= 4, sb, pltpu.roll(sr, 4, 0))


def unpack_high(one, two):
    return one, jnp.where(rows_of() >= 5, pltpu.roll(two, 4, 0), pltpu.roll(one, 3, 0)), two


def y_kernel(bm, srm, sbm, zr, zl, ylow, yhigh):
    for out, row, pack in ((ylow, 0, pack_low), (yhigh, NY - 8, pack_high)):
        for q in range(Q):
            out[q], out[8 + q] = pack(*(ref[q, row + 16:row + 24, :] for ref in (bm, srm, sbm)))
        out[16] = zr[row:row + 8, :]
        out[17] = zl[row:row + 8, :]


def put_rim(rows, r, l, place, refs):
    lane = lanes_of()
    col, half = lane % 16, lane % 64
    parts = [
        turn(jnp.where(col < 12, r, l), -place),
        turn(jnp.where(col < 6, l, r), -place - 6),
        turn(jnp.where(col < 11, l, r), -place - 11),
    ]
    for n, (ref, width) in enumerate(zip(refs, (6, 5, 4))):
        ref[rows, :] = jnp.where(half < width, parts[n], jnp.where(half >= 64 - width, parts[(n + 1) % 3], 0.0))


def edges_low(r, l):
    return jnp.where(lanes_of() < 60, r, turn(l, 64))


def edges_high(r, l):
    return jnp.where(lanes_of() < 60, turn(r, 64), l)


def put_halo_rims(rows, low, high, refs):
    lane = lanes_of()
    high = turn(high, 64)
    r = jnp.where(lane < 60, low, high)
    l = turn(jnp.where((lane >= 60) & (lane < 124), low, high), 64)
    for d in range(3):
        put_rim(rows, r, l, 16 * d, [ref.at[d] for ref in refs[:3 if d < 2 else 2]])


def edge_kernel(after, zr, zl, high, low):
    del after

    def body(first, tiles):
        for u in range(tiles):
            rows = pl.ds(pl.multiple_of((first + u) * 8, 8), 8)
            low[rows, :] = edges_low(zr[rows, :], zl[rows, :])
            high[rows, :] = edges_high(zr[rows, :], zl[rows, :])

    batched(TILES, 16, body)


def corner_kernel(yr, yl, bm_in, srm_in, sbm_in, bh_in, srh_in, sbh_in, high, low, bm, srm, sbm, bh, srh, sbh):
    del bm_in, srm_in, sbm_in, bh_in, srh_in, sbh_in
    for side, (ref, row, unpack) in enumerate(((yr, NY + 16, unpack_low), (yl, 8, unpack_high))):
        for q in range(Q):
            values = unpack(ref[q], ref[8 + q])
            for array, v in zip((bm, srm, sbm), values):
                array[q, row:row + 8, :] = v
            out, d = (low, q) if q < 4 else (high, Q - 1 - q)
            if d < 3:
                out[8 * side + d], out[8 * side + 3 + d] = values[:2]
            if d < 2:
                out[8 * side + 6 + d] = values[2]
        low[16 + side] = edges_low(ref[16], ref[17])
        high[16 + side] = edges_high(ref[16], ref[17])
        for a in range(4):
            put_rim(pl.ds(row, 8), ref[16], ref[17], 16 * a, [rim.at[a] for rim in (bh, srh, sbh)])


class Marks:
    def __init__(self, flip):
        self.lane = lanes_of()
        self.odd = (odd_cells() + flip) % 2 == 1
        turned = (self.lane >= 32) & (self.lane < 96)
        self.rim_odd = self.odd != turned
        self.turned = turned


def half_sweep(r, red, jobs, marks, main, rim, wall, rims=True):
    src, dst, add = ("black", "red", "sr") if red else ("red", "black", "sb")
    lane, odd, rim_odd = marks.lane, marks.odd, marks.rim_odd
    first, last, middle, before = lane == 0, lane == 127, lane == 64, lane == 63
    rows, above, below = pl.ds(r, 8), pl.ds(r - 1, 8), pl.ds(r + 1, 8)
    seen = {}

    def plane(q):
        if q not in seen:
            seen[q] = main(src, q)[rows, :]
        return seen[q]

    def edge(a):
        if ("rim", a) not in seen:
            seen["rim", a] = rim(src, a)[rows, :]
        return seen["rim", a]

    def pick(mark, up, down):
        return jnp.where(mark, up, down) if red else jnp.where(mark, down, up)

    done = {}
    for a, x, keep in jobs:
        b = Q - 1 - a
        turns = [(turn(v, 1), turn(v, 127)) for v in (plane(a), plane(b), edge(a))]
        (l0, r0), (l1, r1), (l2, r2) = turns
        beside = [
            jnp.where(first, l2, l0) + jnp.where(last, r2, r0),
            jnp.where(middle, l2, l1) + jnp.where(before, r2, r1),
        ]
        if rims:
            beside.append(
                jnp.where(first, l0, jnp.where(middle, l1, l2)) + jnp.where(last, r0, jnp.where(before, r1, r2))
            )
        inward = [lambda: plane(a + 1), lambda: plane(b - 1), lambda: edge(a + 1)]
        if a == 3:
            inward = [lambda: turn(plane(4), 64), lambda: turn(plane(3), 64), lambda: turn(edge(3), 64)]
        outward = [lambda: plane(a - 1), lambda: plane(b + 1), lambda: edge(a - 1)]
        refs = [main(src, a), main(src, b), rim(src, a)]
        adds = [main(add, a), main(add, b), rim(add, a)]
        olds = [main(dst, a), main(dst, b), rim(dst, a)]
        new = []
        for n in range(3 if rims else 2):
            if x == "up":
                along = inward[n]()
            elif x == "down":
                along = outward[n]()
            elif n == 1:
                along = pick(odd, outward[n](), inward[n]())
            else:
                along = pick(rim_odd if n == 2 else odd, inward[n](), outward[n]())
            total = (adds[n][rows, :] + (plane(a), plane(b), edge(a))[n]) + (along + beside[n])
            total = total + (refs[n][above, :] + refs[n][below, :])
            value = total * (SIXTH if a >= 0 else wall[n])
            if keep is not None:
                held = [odd, ~odd, rim_odd][n] if keep == 1 else [~odd, odd, ~rim_odd][n]
                value = jnp.where(held, olds[n][rows, :], value)
            new.append(value)
        done[a] = new
    return done


EVERY = ((0, TILES + 2),)


def sweep_rows(red, jobs, marks, main, rim, wall, spans=EVERY):
    dst = "red" if red else "black"

    def body(first, tiles):
        fresh = []
        for u in range(tiles):
            r = pl.multiple_of((first + u) * 8 + 8, 8)
            fresh.append((r, half_sweep(r, red, jobs, marks, main, rim, wall)))
        for r, done in fresh:
            for a, new in done.items():
                for ref, value in zip((main(dst, a), main(dst, Q - 1 - a), rim(dst, a)), new):
                    ref[pl.ds(r, 8), :] = value

    for start, count in spans:
        batched(count, max(1, BATCH // len(jobs)), lambda first, tiles: body(start + first, tiles))


def full(*planes):
    return [(a, "both", None) for a in planes]


INNER = (
    (True, [(0, "up", None)] + full(1, 2, 3)),
    (False, full(1, 2, 3)),
    (True, [(1, "up", 0)] + full(2, 3)),
    (False, full(2, 3)),
    (True, [(2, "up", 0)] + full(3)),
    (False, full(3)),
)
EARLY = 1


def lookups(mains, edges):
    def main(kind, q):
        return mains[kind].at[q]

    def rim(kind, a):
        return edges[kind].at[a]

    return main, rim


def early_kernel(flip_ref, after, zr, zl, bm_in, srm, sbm, bm, rm, bh, rh, srh, sbh):
    del after, bm_in
    marks = Marks(flip_ref[0] % 2)

    def body(first, tiles):
        for u in range(tiles):
            r = pl.multiple_of((first + u) * 8, 8)
            for a in range(4):
                refs = [ref.at[a] for ref in (bh, srh, sbh)]
                put_rim(pl.ds(pl.multiple_of(r + 16, 8), 8), zr[pl.ds(r, 8), :], zl[pl.ds(r, 8), :], 16 * a, refs)

    batched(TILES, 8, body)
    main, rim = lookups({"black": bm, "red": rm, "sr": srm, "sb": sbm}, {"black": bh, "red": rh, "sr": srh, "sb": sbh})
    for n, (red, jobs) in enumerate(INNER[:EARLY]):
        sweep_rows(red, jobs, marks, main, rim, None, ((2 + n, TILES - 2 - 2 * n),))


def inner_kernel(flip_ref, bm_in, rm_in, srm, sbm, bh_in, rh_in, srh, sbh, bm, rm, bh, rh):
    del bm_in, rm_in, bh_in, rh_in
    marks = Marks(flip_ref[0] % 2)
    main, rim = lookups({"black": bm, "red": rm, "sr": srm, "sb": sbm}, {"black": bh, "red": rh, "sr": srh, "sb": sbh})
    for n, (red, jobs) in enumerate(INNER):
        spans = ((0, 2 + n), (TILES - n, 2 + n)) if n < EARLY else EVERY
        sweep_rows(red, jobs, marks, main, rim, None, spans)


def halo_kernel(after, ehigh, elow, xbh, xsrh, xsbh):
    del after

    def body(first, tiles):
        for u in range(tiles):
            r = pl.multiple_of((first + u) * 8, 8)
            put = pl.ds(pl.multiple_of(r + 16, 8), 8)
            put_halo_rims(put, elow[pl.ds(r, 8), :], ehigh[pl.ds(r, 8), :], (xbh, xsrh, xsbh))

    batched(TILES, 16, body)


OUT_CHUNKS = 4


SLOTS = {"black": 0, "sr": 3, "sb": 6}


def outer_kernel(flip_ref, bm_in, rm_in, srm, sbm, bh_in, rh_in, srh, sbh, chigh, clow,
                 low_in, high_in, xbh_in, xsrh_in, xsbh_in,
                 out, bm, rm, bh, rh, low, high, xbh, xsrh, xsbh, xrm, xrh, obuf, sems):
    del bm_in, rm_in, bh_in, rh_in, low_in, high_in, xbh_in, xsrh_in, xsbh_in
    flip = flip_ref[0] % 2
    marks = Marks(flip)
    outside = jnp.where(flip_ref[0] >= 2, 0.0, SIXTH)
    wall = (outside, SIXTH, jnp.where(marks.turned, SIXTH, outside))
    plain = odd_cells() == 1

    for y, (row, n) in enumerate(((NY + 16, 0), (8, 8))):
        for face, corner in ((low, clow), (high, chigh)):
            for slot in range(8):
                face[slot, row:row + 8, :] = corner[n + slot]
        put_halo_rims(pl.ds(row, 8), clow[16 + y], chigh[16 + y], (xbh, xsrh, xsbh))

    mains = {"black": bm, "red": rm, "sr": srm, "sb": sbm}
    edges = {"black": (bh, xbh), "red": (rh, xrh), "sr": (srh, xsrh), "sb": (sbh, xsbh)}

    def main(kind, q):
        if 0 <= q < Q:
            return mains[kind].at[q]
        d = -1 - q if q < 0 else q - Q
        if kind == "red":
            return xrm.at[d if q < 0 else 3 + d]
        return (low if q < 0 else high).at[SLOTS[kind] + d]

    def rim(kind, a):
        own, halo = edges[kind]
        return own.at[a] if a >= 0 else halo.at[-1 - a]

    for red, jobs in (
        (True, [(-3, "up", None)] + full(-2, -1) + [(0, "down", 1)]),
        (False, full(-2, -1, 0)),
        (True, [(-2, "up", None)] + full(-1, 0) + [(1, "down", 1)]),
        (False, full(-1, 0, 1)),
        (True, [(-1, "up", None)] + full(0, 1) + [(2, "down", 1)]),
    ):
        sweep_rows(red, jobs, marks, main, rim, wall)

    def tiles(i, carry):
        done = []
        for u in range(8):
            t = i * 8 + u
            r = pl.multiple_of(t * 8 + 16, 8)
            done.append((t, r, half_sweep(r, False, full(0, 1, 2), marks, main, rim, wall, rims=False)))
        for t, r, new in done:
            rows = pl.ds(pl.multiple_of(t * 8, 8), 8)
            for q in range(Q):
                a = min(q, Q - 1 - q)
                b = new[a][0 if q == a else 1] if a in new else bm[q, pl.ds(r, 8), :]
                v = rm[q, pl.ds(r, 8), :]
                at = mirrored(q, flip)
                for n, value in enumerate((jnp.where(plain, b, v), jnp.where(plain, v, b))):
                    obuf[at, n, rows, :] = value if q < 4 else turn(value, 64)
        return carry

    span = NY // OUT_CHUNKS
    copies = []
    for c in range(OUT_CHUNKS):
        lax.fori_loop(c * span // 64, (c + 1) * span // 64, tiles, 0)
        rows = pl.ds(c * span, span)
        copy = pltpu.make_async_copy(obuf.at[:, :, rows, :], out.at[:, :, rows, :], sems.at[c])
        copy.start()
        copies.append(copy)
    for copy in copies:
        copy.wait()


def smem():
    return pl.BlockSpec(memory_space=pltpu.SMEM)


def hbm():
    return pl.BlockSpec(memory_space=pl.ANY)


def near(value):
    return pltpu.with_memory_space_constraint(value, VM)


def room(mib):
    return pltpu.CompilerParams(vmem_limit_bytes=mib * 1024 * 1024)


def ring(size, step):
    return [(i, (i + step) % size) for i in range(size)]


def kernel(body, mib, outs, ins, **more):
    pairs = [i if isinstance(i, tuple) else (near(i), pl.BlockSpec(memory_space=VM)) for i in ins]
    arrays, specs = zip(*pairs)
    out_specs = more.pop("out_specs", [pl.BlockSpec(memory_space=VM)] * len(outs))
    return pl.pallas_call(
        body, out_shape=outs, in_specs=specs, out_specs=out_specs, compiler_params=room(mib), **more
    )(*arrays)


def send(value, axis, pairs):
    return lax.ppermute(near(value), axis, pairs)


def all_sweeps(field, source):
    gx = lax.axis_index("gx")
    last = lax.axis_size("gx") - 1
    walled = (gx == 0) | (gx == last)
    flip = (gx % 2 + 2 * walled.astype(jnp.int32))[None], smem()
    pairs = lax.axis_size("gx") // 2
    chip = [p for i in range(pairs) for p in ((2 * i, 2 * i + 1), (2 * i + 1, 2 * i))]
    across = [p for i in range(pairs - 1) for p in ((2 * i + 1, 2 * i + 2), (2 * i + 2, 2 * i + 1))]
    ny, nz = lax.axis_size("gy"), lax.axis_size("gz")

    blocks = [
        (pltpu.with_memory_space_constraint(a.reshape(Q, 2, NY, NZ), pltpu.HBM), hbm()) for a in (field, source)
    ]
    edge = VM((4, ROWS, NZ), F32)
    work, block = VM((Q, ROWS, NZ), F32), VM((Q, 2, NY, NZ), F32)
    rows, strip, corner = VM((NY, NZ), F32), VM((18, 8, NZ), F32), VM((18, 8, NZ), F32)

    fbuf, sbuf, zlow, zhigh = kernel(
        pack_kernel, 2, (block, block, rows, rows), [flip] + blocks,
        scratch_shapes=[pltpu.SemaphoreType.DMA((2 * CHUNKS,))],
    )
    zr = send(zlow, "gz", ring(nz, -1))
    zl = send(zhigh, "gz", ring(nz, 1))
    bm, srm, sbm, high, low = kernel(face_kernel, 2, (work,) * 5, [flip, fbuf, sbuf])
    high = send(high, "gx", chip)
    low = send(low, "gx", across)
    ylow, yhigh = kernel(y_kernel, 2, (strip, strip), [bm, srm, sbm, zr, zl])
    yr = send(ylow, "gy", ring(ny, -1))
    yl = send(yhigh, "gy", ring(ny, 1))
    ehigh, elow = kernel(edge_kernel, 2, (rows, rows), [(ylow, hbm()), zr, zl])
    ehigh = send(ehigh, "gx", chip)
    elow = send(elow, "gx", across)
    bm, rm, bh, rh, srh, sbh = kernel(
        early_kernel, 4, (work, work) + (edge,) * 4, [flip, (ylow, hbm()), zr, zl, bm, srm, sbm],
        input_output_aliases={4: 0},
    )
    chigh, clow, bm, srm, sbm, bh, srh, sbh = kernel(
        corner_kernel, 2, (corner, corner) + (work,) * 3 + (edge,) * 3, [yr, yl, bm, srm, sbm, bh, srh, sbh],
        input_output_aliases={2 + i: 2 + i for i in range(6)},
    )
    turn_of_halo = clow
    chigh = send(chigh, "gx", chip)
    clow = send(clow, "gx", across)
    bm, rm, bh, rh = kernel(
        inner_kernel, 4, (work, work, edge, edge), [flip, bm, rm, srm, sbm, bh, rh, srh, sbh],
        input_output_aliases={1: 0, 2: 1, 5: 2, 6: 3},
    )
    red, *halo = [VM((n, ROWS, NZ), F32) for n in (6, 3, 3, 2)]
    halos = kernel(halo_kernel, 2, halo, [(turn_of_halo, hbm()), ehigh, elow])
    out = kernel(
        outer_kernel, 12,
        [jax.ShapeDtypeStruct((Q, 2, NY, NZ), F32), work, work, edge, edge, work, work] + halo,
        [flip, bm, rm, srm, sbm, bh, rh, srh, sbh, chigh, clow, low, high, *halos],
        out_specs=[hbm()] + [pl.BlockSpec(memory_space=VM)] * 9,
        input_output_aliases={1: 1, 2: 2, 5: 3, 6: 4, **{11 + i: 5 + i for i in range(5)}},
        scratch_shapes=[red, halo[0], block, pltpu.SemaphoreType.DMA((OUT_CHUNKS,))],
    )[0]
    return out.reshape(field.shape)


def solution(mesh):
    spec = P("gx", "gy", "gz")
    return jax.shard_map(all_sweeps, mesh=mesh, in_specs=(spec, spec), out_specs=spec, check_vma=False)
```
